16 devices in a mesh: dp: 2 (over y, z), tp: 8 (over x, core).
Axes of the slice: x: 4, y: 2, z: 1, core: 2. Of those that a mesh axis runs over, the one named last changes fastest.
The devices are a block of a 4x4x8 slice.
Arguments:
- x: bfloat16 [8, 512, 5120], P('dp'), parts along dimension 0
- gain_a: bfloat16 [5120], replicated
- wq: bfloat16 [5120, 4096], P(None, 'tp')
- wk: bfloat16 [5120, 1024], P(None, 'tp')
- wv: bfloat16 [5120, 1024], P(None, 'tp')
- wo: bfloat16 [4096, 5120], P('tp')
- gain_m: bfloat16 [5120], replicated
- w_gate: bfloat16 [5120, 32768], P(None, 'tp')
- w_up: bfloat16 [5120, 32768], P(None, 'tp')
- w_down: bfloat16 [32768, 5120], P('tp')
Outputs:
- output: bfloat16 [8, 512, 5120], P('dp'), parts along dimension 0
There are 2 independent parts. The reference program is written for one: setup_inputs(seed, part) draws one part's arguments, and reference() takes and returns one part's arrays. A program takes and returns all parts, laid end to end along the dimension named above; an argument that names none is the same for every part.
All inputs are finite; a program needn't handle non-finite values.
Results may differ from the reference program's by a relative error of at most 0.017.
Values are sent between devices in bfloat16 or wider.
A program may use at most 768 MiB of HBM per device.

```python
import jax
import jax.numpy as jnp
from jax import lax

SEQUENCES = 4
TOKENS = 512
D = 5120
HEADS = 32
KV_HEADS = 8
HEAD = 128
FF = 32768
THETA = 10000


def setup_inputs(seed: int = 0, part: int = 0) -> dict:
    kx, ka, km, kq, kk, kv, ko, kg, ku, kd = jax.random.split(jax.random.key(seed), 10)

    def weights(key, rows, columns):
        return jax.random.normal(key, (rows, columns), jnp.float32) * rows**-0.5

    drawn = {
        "x": jax.random.normal(jax.random.fold_in(kx, part), (SEQUENCES, TOKENS, D), jnp.float32),
        "gain_a": 1 + 0.1 * jax.random.normal(ka, (D,), jnp.float32),
        "wq": 2 * weights(kq, D, HEADS * HEAD),
        "wk": 2 * weights(kk, D, KV_HEADS * HEAD),
        "wv": 4 * weights(kv, D, KV_HEADS * HEAD),
        "wo": weights(ko, HEADS * HEAD, D),
        "gain_m": 1 + 0.1 * jax.random.normal(km, (D,), jnp.float32),
        "w_gate": weights(kg, D, FF),
        "w_up": weights(ku, D, FF),
        "w_down": 3 * weights(kd, FF, D),
    }
    return {k: v.astype(jnp.bfloat16) for k, v in drawn.items()}


def normed(x, gain):
    wide = x.astype(jnp.float32)
    scale = lax.rsqrt(jnp.mean(wide * wide, -1, keepdims=True) + 1e-6)
    return (wide * scale * gain.astype(jnp.float32)).astype(jnp.bfloat16)


def turned(t, place, theta):
    half = t.shape[-1] // 2
    angle = place.astype(jnp.float32)[:, None] * theta ** (-jnp.arange(half, dtype=jnp.float32) / half)
    cos, sin = jnp.cos(angle)[:, None], jnp.sin(angle)[:, None]
    a, b = t[..., :half].astype(jnp.float32), t[..., half:].astype(jnp.float32)
    return jnp.concatenate([a * cos - b * sin, b * cos + a * sin], -1).astype(jnp.bfloat16)


def matmul(a, w):
    return jnp.dot(a, w, preferred_element_type=jnp.float32).astype(jnp.bfloat16)


def einsum(form, a, b):
    return jnp.einsum(form, a.astype(jnp.float32), b.astype(jnp.float32))


def attention(q, k, v):
    scores = einsum("tgsd,ugd->gstu", q, k) * q.shape[-1] ** -0.5
    token = jnp.arange(q.shape[0])
    scores = jnp.where(token[:, None] >= token, scores, -jnp.inf)
    weights = jax.nn.softmax(scores, -1).astype(jnp.bfloat16)
    return einsum("gstu,ugd->tgsd", weights, v).astype(jnp.bfloat16)


def one(x, gain_a, wq, wk, wv, wo, gain_m, w_gate, w_up, w_down):
    rows = x.shape[0]
    a, place = normed(x, gain_a), jnp.arange(rows)
    k = turned(matmul(a, wk).reshape(rows, -1, HEAD), place, THETA)
    q = turned(matmul(a, wq).reshape(rows, -1, HEAD), place, THETA).reshape(rows, k.shape[1], -1, HEAD)
    v = matmul(a, wv).reshape(rows, -1, HEAD)
    seen = attention(q, k, v).reshape(rows, -1)
    h = (x.astype(jnp.float32) + jnp.dot(seen, wo, preferred_element_type=jnp.float32)).astype(jnp.bfloat16)
    b = normed(h, gain_m)
    gate = jnp.dot(b, w_gate, preferred_element_type=jnp.float32)
    up = jnp.dot(b, w_up, preferred_element_type=jnp.float32)
    hidden = (jax.nn.silu(gate) * up).astype(jnp.bfloat16)
    return (h.astype(jnp.float32) + jnp.dot(hidden, w_down, preferred_element_type=jnp.float32)).astype(jnp.bfloat16)


def reference(x, gain_a, wq, wk, wv, wo, gain_m, w_gate, w_up, w_down):
    return lax.map(lambda sequence: one(sequence, gain_a, wq, wk, wv, wo, gain_m, w_gate, w_up, w_down), x)
```

```python
import functools

import jax
import jax.numpy as jnp
from jax import lax
from jax.experimental import pallas as pl
from jax.experimental.pallas import tpu as pltpu
from jax.sharding import PartitionSpec as P

HEAD = 128
THETA = 10000
JOB = 256
TG = 256
TD = 512
SLOTS = 4
HALVES = 2
CHUNKS = (1, 1, 2, 2, 1, 1)
PLAN_FIRST = ((34949120, 1131010), (33554432, 332880))
PLAN_CHUNKS = (
    ((15, 8), (0, 0), ((17125478, 6702101), (20972802, 1466624)), 0),
    ((37, 22), (0, 0), ((22025297, 418820), (1377286, 21063236)), 0),
    ((53, 40), (0, 0), ((27874646, 5342305), (23745621, 42475848)), 1),
    ((80, 67), (0, 0), ((42551464, 0), (43078954, 104038)), 1),
    ((96, 96), (0, 0), ((22369440, 85), (0, 22303880)), 1),
    ((112, 107), (0, 0), ((21304328, 0), (33554773, 4473152)), 0),
)
PLAN_TAIL = ((120, 119), 17, 130561)
HIDDEN = -1e30
F32, BF16 = jnp.float32, jnp.bfloat16


def _dot(a, b, ca=1, cb=0):
    return lax.dot_general(a, b, (((ca,), (cb,)), ((), ())), preferred_element_type=F32)


def _ds(start, size, unit=128):
    return pl.ds(pl.multiple_of(start, unit), size)


def _kernel(n, rows, length, d, heads, ff, *refs):
    (x, ga, wq, wk, wv, wo, gm, wg, wu, wd, G, town, tpar,
     tv_own, tv_par, xres, rrecv, rsend, fin, gout, hown, wbuf,
     exch_recv, agp_recv, rs_recv, rs_send, ag_recv, ag_sn, ag_sp, agl, tl, gsem, bsem, osem, psem, wsem, xsem, gains) = refs
    chips, half, blk, cw = n // 2, JOB // 2, JOB // n, d // HALVES
    nj = rows // JOB
    per = HALVES * chips
    half_plan = 13
    qw = heads * HEAD
    me = lax.axis_index("tp")
    chip, core = me // 2, me % 2
    step = 1 - 2 * core
    at = lambda c, k: ((c + chips) % chips) * 2 + k
    nxt, prv, partner = at(chip + step, core), at(chip - step, core), at(chip, 1 - core)

    barrier = pltpu.get_barrier_semaphore()
    for other in (nxt, prv, partner):
        pl.semaphore_signal(barrier, inc=1, device_id={"tp": other}, device_id_type=pl.DeviceIdType.MESH)

    gains[0:1] = ga[...].astype(F32).reshape(1, d)
    gains[1:2] = gm[...].astype(F32).reshape(1, d)

    def remote(src, dst, send, recv, to):
        return pltpu.make_async_remote_copy(src_ref=src, dst_ref=dst, send_sem=send, recv_sem=recv, device_id={"tp": to},
                                            device_id_type=pl.DeviceIdType.MESH)

    local = pltpu.make_async_copy

    def event(e):
        alone = (e < 2 * per) | (e >= (nj - 1) * 2 * per)
        both = lax.rem(e, 2 * per)
        j = jnp.where(alone, lax.div(e, per), 2 * lax.div(e, 2 * per) + lax.div(lax.rem(both, 2 * HALVES), HALVES))
        return j, jnp.where(alone, lax.div(lax.rem(e, per), HALVES), lax.div(both, 2 * HALVES)), lax.rem(e, HALVES)

    def last_event(j):
        alone = (j < 2) | (j >= 2 * nj - 2)
        return per * j + per - 1 + jnp.where(alone | (lax.rem(j, 2) == 1), 0, per - HALVES)

    def loads(j):
        p = j % 2
        mine = _ds((j % nj) * JOB + core * half + chip * blk, blk, blk)
        return (local(town.at[j], tv_own.at[p], tl.at[p, 0]), local(tpar.at[j], tv_par.at[p], tl.at[p, 1]),
                local(x.at[mine], xres.at[p], tl.at[p, 2]))

    def exchanged(j):
        return remote(tpar.at[j], tpar.at[j], psem.at[0, 0], exch_recv.at[j], partner)

    def tload(j):
        exchanged(j).wait_recv()
        for c in loads(j):
            c.start()

    def ring(j, r, c):
        return remote(rsend.at[j % 2, r, c], rrecv.at[j % 4, r, c], rs_send.at[j % 2, r, c], rs_recv.at[j % 4, r, c], nxt)

    def finish(j):
        idx, p = j % nj, j % 2

        @pl.when(j < nj)
        def _():
            h = (xres[p].astype(F32) + fin[...]).astype(BF16)
            hown[idx] = h
            wide = h.astype(F32)
            scale = lax.rsqrt(jnp.mean(wide * wide, -1, keepdims=True) + 1e-6)
            gout[j % 4] = (wide * scale * gains[1:2]).astype(BF16)

        @pl.when(j >= nj)
        def _():
            gout[j % 4] = (hown[idx].astype(F32) + fin[...]).astype(BF16)

    def rs_event(e, avail):
        j, r, c = event(e)
        p = lax.rem(j, 2)
        o = lax.rem(chip + step * (chips - 1 - r) + chips * 2, chips)
        there, cols = _ds(o * blk, blk, blk), _ds(c * cw, cw)

        @pl.when((r == 0) & (c == 0))
        def _():
            for copy in loads(j):
                copy.wait()

        def both():
            return tv_own[p, there, cols] + tv_par[p, there, cols].astype(F32)

        def send(value):
            @pl.when(j >= 2)
            def _():
                ring(j - 2, r, c).wait_send()

            rsend[p, r, c] = value.astype(BF16)
            ring(j, r, c).start()

        @pl.when(r == 0)
        def _():
            send(both())

        @pl.when(r > 0)
        def _():
            ring(j, r - 1, c).wait_recv()

        @pl.when((r > 0) & (r < chips - 1))
        def _():
            send(both() + rrecv[j % 4, r - 1, c].astype(F32))

        @pl.when(r == chips - 1)
        def _():
            fin[:, cols] = both() + rrecv[j % 4, r - 1, c].astype(F32)

        @pl.when((r == chips - 1) & (c == HALVES - 1))
        def _():
            finish(j)

            @pl.when(j + 2 <= avail)
            def _():
                tload(j + 2)

    def block(j, g):
        o = lax.rem(chip - step * g + chips * 2, chips)
        return _ds(j * JOB + core * half + o * blk, blk, blk)

    def to_next(j, g, c, src):
        return remote(src, G.at[block(j, g), _ds(c * cw, cw)], ag_sn.at[j % 2, g, c], ag_recv.at[j % 8, g, c], nxt)

    def to_partner(j, g, c, src):
        return remote(src, G.at[block(j, g), _ds(c * cw, cw)], ag_sp.at[j % 2, g, c], agp_recv.at[j], partner)

    def keep(j, c):
        return local(gout.at[j % 4, :, _ds(c * cw, cw)], G.at[block(j, 0), _ds(c * cw, cw)], agl.at[j % 2, c])

    def ag_event(e):
        j, g, c = event(e)
        here = G.at[block(j, g), _ds(c * cw, cw)]

        @pl.when(j >= 2)
        def _():
            to_partner(j - 2, g, c, here).wait_send()

            @pl.when(g < chips - 1)
            def _():
                to_next(j - 2, g, c, here).wait_send()

        @pl.when(g == 0)
        def _():
            mine = gout.at[j % 4, :, _ds(c * cw, cw)]
            to_next(j, g, c, mine).start()
            to_partner(j, g, c, mine).start()
            keep(j, c).start()

        @pl.when(g > 0)
        def _():
            to_next(j, g - 1, c, here).wait_recv()

            @pl.when(g < chips - 1)
            def _():
                to_next(j, g, c, here).start()

            to_partner(j, g, c, here).start()

        @pl.when(g == chips - 1)
        def _():
            keep(j, c).wait()

    def gathered(j):
        there = G.at[_ds(j * JOB, half, half)]
        remote(there, there, ag_sp.at[0, 0, 0], agp_recv.at[j], partner).wait_recv()

    def pump(plan, t, at_, avail):
        (a0, a1), (b0, b1) = plan
        u = 2 * lax.rem(t, half_plan)
        a = lax.shift_right_logical(jnp.where(t < half_plan, a0, a1), u) & 3
        b = lax.shift_right_logical(jnp.where(t < half_plan, b0, b1), u) & 3
        r, g = at_
        lax.fori_loop(r, r + a, lambda e, _: rs_event(e, avail), None)
        lax.fori_loop(g, g + b, lambda e, _: ag_event(e), None)
        return r + a, g + b

    def catch_up(j, at_):
        @pl.when((j < 2) | (last_event(j - 2) < at_[0]))
        def _():
            tload(j)

    n1, n2 = ff // TG, d // TD
    ticks = n1 + n2
    tiles = ticks * len(CHUNKS)
    slot_of = lambda T: (T + 3) % SLOTS

    def g_copies(T):
        col, s = _ds((T % ticks) * TG, TG), slot_of(T)
        return (local(wg.at[:, col], wbuf.at[s, :, pl.ds(0, TG)], gsem.at[s, 0]),
                local(wu.at[:, col], wbuf.at[s, :, pl.ds(TG, TG)], gsem.at[s, 1]))

    def d_copy(T):
        return local(wd.at[:, _ds((T % ticks - n1) * TD, TD)], wbuf.at[slot_of(T), pl.ds(0, ff)], gsem.at[slot_of(T), 0])

    def fetch(T):
        @pl.when((T % ticks < n1) & (T < tiles))
        def _():
            for c in g_copies(T):
                c.start()

        @pl.when((T % ticks >= n1) & (T < tiles))
        def _():
            d_copy(T).start()

    def first(xb, ab, qb, kb, vb, seen, own_st, par_st, cos, sin):
        nh = rows // JOB
        up = length // JOB
        wcopies = [local(wq, wbuf.at[0], wsem.at[0]), local(wk, wbuf.at[1, :, pl.ds(0, HEAD)], wsem.at[1]),
                   local(wv, wbuf.at[1, :, pl.ds(HEAD, HEAD)], wsem.at[2])]
        wcopies += [local(wo.at[:, pl.ds(t * TD, TD)], wbuf.at[2, pl.ds(t * qw, qw)], wsem.at[3 + t]) for t in range(n2)]
        x_copy = lambda h: local(x.at[_ds(h * JOB, JOB, JOB)], xb.at[h % 2], xsem.at[h % 2])
        x_copy(0).start()
        for c in wcopies[:3]:
            c.start()
        lane = lax.broadcasted_iota(jnp.int32, (16, HEAD), 1)
        row = lax.broadcasted_iota(jnp.int32, (16, HEAD), 0).astype(F32)
        power = jnp.exp((lane % (HEAD // 2)).astype(F32) * (-2.0 / HEAD) * jnp.log(jnp.float32(THETA)))
        sign = jnp.where(lane < HEAD // 2, -1.0, 1.0)
        cf, sf = jnp.cos(row * power), jnp.sin(row * power)
        for a in range(0, length, 256):
            cc, sc = jnp.cos((16 * row + a) * power), jnp.sin((16 * row + a) * power)
            for i in range(16):
                at_ = slice(a + 16 * i, a + 16 * (i + 1))
                ci, si = cc[i : i + 1], sc[i : i + 1]
                cos[at_, :] = ci * cf - si * sf
                sin[at_, :] = sign * (si * cf + ci * sf)

        def out(h):
            return (local(own_st, town.at[h], osem.at[0, 0]), remote(par_st, tpar.at[h], psem.at[0, 0], exch_recv.at[h], partner))

        def normed(h):
            for a in range(0, JOB, 16):
                rows_ = slice(a, a + 16)
                wide = xb[h % 2, rows_, :].astype(F32)
                scale = lax.rsqrt(jnp.mean(wide * wide, -1, keepdims=True) + 1e-6)
                ab[h % 2, rows_, :] = (xb[h % 2, rows_, :].astype(F32) * scale * gains[0:1]).astype(BF16)

        x_copy(1).start()
        x_copy(0).wait()
        normed(0)
        for c in wcopies[:3]:
            c.wait()
        for c in wcopies[3:]:
            c.start()

        pl.semaphore_wait(barrier, 3)

        def body(h, at_):
            at_seq = (h % up) * JOB

            @pl.when(h + 1 < nh)
            def _():
                x_copy(h + 1).wait()

            here = _ds(at_seq, JOB, JOB)
            cosv, sinv = cos[here, :], sin[here, :]

            def turned(t):
                t = t.astype(BF16).astype(F32)
                return (t * cosv + pltpu.roll(t, HEAD // 2, 1) * sinv).astype(BF16)

            queries = _dot(ab[h % 2], wbuf[0])
            others = _dot(ab[h % 2], wbuf[1, :, : 2 * HEAD])
            normed(h + 1)
            kb[here, :] = turned(others[:, :HEAD])
            vb[here, :] = others[:, HEAD:].astype(BF16)
            for m in range(heads):
                qb[:, m * HEAD : (m + 1) * HEAD] = turned(queries[:, m * HEAD : (m + 1) * HEAD])

            @pl.when(h + 2 < nh)
            def _():
                x_copy(h + 2).start()

            @pl.when(h == nh - 1)
            def _():
                fetch(1)
                fetch(2)

            @pl.when(h == 0)
            def _():
                for c in wcopies[3:]:
                    c.wait()

            @pl.when(h == 3)
            def _():
                fetch(0)

            at_ = pump(PLAN_FIRST, 3 * h, at_, h - 2)

            def attend(keys):
                ok = (keys - JOB + lax.broadcasted_iota(jnp.int32, (JOB, keys), 0)) >= lax.broadcasted_iota(jnp.int32, (JOB, keys), 1)
                for m in range(heads):
                    s = _dot(qb[:, m * HEAD : (m + 1) * HEAD], kb[:keys], 1, 1) * HEAD**-0.5
                    s = jnp.where(ok, s, HIDDEN)
                    w = jnp.exp(s - s.max(-1, keepdims=True))
                    total = w.sum(-1, keepdims=True)
                    seen[:, m * HEAD : (m + 1) * HEAD] = (_dot(w.astype(BF16), vb[:keys]) / total).astype(BF16)

            for part in range(up):
                @pl.when(h % up == part)
                def _():
                    attend((part + 1) * JOB)

            @pl.when(h >= 1)
            def _():
                own, par = out(h - 1)
                own.wait()
                par.wait_send()

            @pl.when(h >= 1)
            def _():
                catch_up(h - 1, at_)

            at_ = pump(PLAN_FIRST, 3 * h + 1, at_, h - 1)

            for t in range(n2):
                cols = slice(t * TD, (t + 1) * TD)
                val = _dot(seen[...], wbuf[2, t * qw : (t + 1) * qw])
                v0, v1 = val[:half], val[half:]
                own_st[:, cols] = jnp.where(core == 0, v0, v1)
                par_st[:, cols] = jnp.where(core == 0, v1, v0).astype(BF16)
            for c in out(h):
                c.start()
            return pump(PLAN_FIRST, 3 * h + 2, at_, h - 1)

        lax.fori_loop(0, nh, body, (jnp.int32(0), jnp.int32(0)))
        own, par = out(nh - 1)
        own.wait()
        par.wait_send()
        catch_up(nh - 1, PLAN_CHUNKS[0][0])

    pl.run_scoped(first, pltpu.VMEM((2, JOB, d), BF16), pltpu.VMEM((2, JOB, d), BF16), pltpu.VMEM((JOB, qw), BF16), pltpu.VMEM((length, HEAD), BF16),
                  pltpu.VMEM((length, HEAD), BF16), pltpu.VMEM((JOB, qw), BF16), pltpu.VMEM((half, d), F32), pltpu.VMEM((half, d), BF16),
                  pltpu.VMEM((length, HEAD), F32), pltpu.VMEM((length, HEAD), F32))


    def second(bb, hid, ost, pst):
        def b_copy(first_job, jobs, s):
            return local(G.at[_ds(first_job * JOB, jobs * JOB, JOB)], bb.at[s, pl.ds(0, jobs * JOB)], bsem)

        def chunk(k, first_job, jobs, at_, plan, mid):
            m = jobs * JOB
            s = k % 2
            avail = nj + first_job - 1

            def g_tile(t, at_):
                T = k * ticks + t
                fetch(T + SLOTS - 1)
                for c in g_copies(T):
                    c.wait()
                r = _dot(bb[s, :m], wbuf[slot_of(T)])
                gate, upv = r[:, :TG], r[:, TG:]
                hid[:m, _ds(t * TG, TG)] = (jax.nn.silu(gate) * upv).astype(BF16)
                return pump(plan, t, at_, avail)

            at_ = lax.fori_loop(0, n1, g_tile, at_)
            mid()

            def outs(t, q):
                col = _ds(t * TD, TD)
                return (local(ost.at[t % 2, q], town.at[nj + first_job + q, :, col], osem.at[t % 2, q]),
                        remote(pst.at[t % 2, q], tpar.at[nj + first_job + q, :, col], psem.at[t % 2, q], exch_recv.at[nj + first_job + q], partner))

            def d_tile(t, at_):
                T = k * ticks + n1 + t
                fetch(T + SLOTS - 1)
                d_copy(T).wait()

                @pl.when(t >= 2)
                def _():
                    for q in range(jobs):
                        own, par = outs(t - 2, q)
                        own.wait()
                        par.wait_send()

                val = _dot(hid[:m], wbuf[slot_of(T), :ff])
                for q in range(jobs):
                    v0, v1 = val[q * JOB : q * JOB + half], val[q * JOB + half : (q + 1) * JOB]
                    ost[t % 2, q] = jnp.where(core == 0, v0, v1)
                    pst[t % 2, q] = jnp.where(core == 0, v1, v0).astype(BF16)
                    for c in outs(t, q):
                        c.start()
                return pump(plan, n1 + t, at_, avail)

            lax.fori_loop(0, n2, d_tile, at_)
            for t in (n2 - 2, n2 - 1):
                for q in range(jobs):
                    own, par = outs(t, q)
                    own.wait()
                    par.wait_send()

        def have(first_job, jobs, s):
            for q in range(jobs):
                gathered(first_job + q)
            b_copy(first_job, jobs, s).start()

        def run(lo, hi):
            jobs = CHUNKS[lo]
            ks = range(lo, hi)

            def body(k, _):
                def pick(f):
                    value = f(lo)
                    for i in ks[1:]:
                        value = jnp.where(k == i, f(i), value) if f(i) != f(lo) else value
                    return jnp.int32(value)

                first_job = pick(lambda i: sum(CHUNKS[:i]))
                r, g = (pick(lambda i: PLAN_CHUNKS[i][0][q]) for q in (0, 1))
                ahead = [pick(lambda i: PLAN_CHUNKS[i][1][q]) for q in (0, 1)]
                plan = [[pick(lambda i: PLAN_CHUNKS[i][2][q][u]) for u in (0, 1)] for q in (0, 1)]
                before = pick(lambda i: CHUNKS[i - 1] if i else 0)
                after = pick(lambda i: CHUNKS[i + 1] if i + 1 < len(CHUNKS) else 0)
                for q in (2, 1):
                    @pl.when(q <= before)
                    def _():
                        catch_up(nj + first_job - q, (r, g))

                lax.fori_loop(r, r + ahead[0], lambda e, _: rs_event(e, nj + first_job - 1), None)
                lax.fori_loop(g, g + ahead[1], lambda e, _: ag_event(e), None)

                @pl.when(pick(lambda i: int(i == 0 or not PLAN_CHUNKS[i - 1][3])) == 1)
                def _():
                    have(first_job, jobs, k % 2)

                b_copy(0, jobs, 0).wait()

                def mid():
                    for q in (1, 2):
                        @pl.when((pick(lambda i: PLAN_CHUNKS[i][3]) == 1) & (after == q))
                        def _():
                            have(first_job + jobs, q, (k + 1) % 2)

                chunk(k, first_job, jobs, (r + ahead[0], g + ahead[1]), plan, mid)

            lax.fori_loop(lo, hi, body, None)

        lo = 0
        for hi in range(1, len(CHUNKS) + 1):
            if hi == len(CHUNKS) or CHUNKS[hi] != CHUNKS[lo]:
                run(lo, hi)
                lo = hi

    pl.run_scoped(second, pltpu.VMEM((2, 2 * JOB, d), BF16), pltpu.VMEM((2 * JOB, ff), BF16),
                  pltpu.VMEM((2, 2, half, TD), F32), pltpu.VMEM((2, 2, half, TD), BF16))

    start, steps, which = PLAN_TAIL
    catch_up(2 * nj - 1, start)

    def tail(t, at_):
        r, g = at_
        gather = lax.shift_right_logical(jnp.int32(which), t) & 1

        @pl.when(gather == 0)
        def _():
            rs_event(r, 2 * nj - 1)

        @pl.when(gather == 1)
        def _():
            ag_event(g)

        return r + 1 - gather, g + gather

    lax.fori_loop(0, steps, tail, (jnp.int32(start[0]), jnp.int32(start[1])))
    for j in (2 * nj - 2, 2 * nj - 1):
        for c in range(HALVES):
            for r in range(chips - 1):
                ring(j, r, c).wait_send()
                to_next(j, r, c, G.at[block(j, r), _ds(c * cw, cw)]).wait_send()
            for g in range(chips):
                to_partner(j, g, c, G.at[block(j, g), _ds(c * cw, cw)]).wait_send()

    def all_here(j, _):
        gathered(j)

    lax.fori_loop(nj, 2 * nj, all_here, None)


def _copy(start, size, src, dst, buf, get, put):
    n = buf.shape[0]
    ins = [pltpu.make_async_copy(src.at[pl.ds(start + i * size, size)], buf.at[i], get.at[i]) for i in range(n)]
    outs = [pltpu.make_async_copy(buf.at[i], dst.at[pl.ds(i * size, size)], put.at[i]) for i in range(n)]
    for c in ins:
        c.start()
    for i in range(n):
        ins[i].wait()
        outs[i].start()
    for c in outs:
        c.wait()


def solution(mesh):
    n = mesh.shape["tp"]
    chips = n // 2

    def step(x, gain_a, wq, wk, wv, wo, gain_m, w_gate, w_up, w_down):
        batch, length, d = x.shape
        rows, heads, ff = batch * length, wq.shape[1] // HEAD, w_gate.shape[1]
        nj, half, blk, cw = rows // JOB, JOB // 2, JOB // n, d // HALVES
        dma, anywhere, vmem = pltpu.SemaphoreType.DMA, pl.BlockSpec(memory_space=pl.ANY), pl.BlockSpec(memory_space=pltpu.VMEM)
        got, _, _ = pl.pallas_call(
            functools.partial(_kernel, n, rows, length, d, heads, ff),
            in_specs=[anywhere, vmem, anywhere, anywhere, anywhere, anywhere, vmem, anywhere, anywhere, anywhere],
            out_specs=[anywhere] * 3,
            out_shape=[jax.ShapeDtypeStruct((2 * rows, d), BF16), jax.ShapeDtypeStruct((2 * nj, half, d), F32),
                       jax.ShapeDtypeStruct((2 * nj, half, d), BF16)],
            scratch_shapes=[
                pltpu.VMEM((2, half, d), F32),
                pltpu.VMEM((2, half, d), BF16),
                pltpu.VMEM((2, blk, d), BF16),
                pltpu.VMEM((4, chips - 1, HALVES, blk, cw), BF16),
                pltpu.VMEM((2, chips - 1, HALVES, blk, cw), BF16),
                pltpu.VMEM((blk, d), F32),
                pltpu.VMEM((4, blk, d), BF16),
                pltpu.VMEM((nj, blk, d), BF16),
                pltpu.VMEM((SLOTS, d, 2 * TG), BF16),
                dma((2 * nj,)),
                dma((2 * nj,)),
                dma((4, chips - 1, HALVES)),
                dma((2, chips - 1, HALVES)),
                dma((8, chips - 1, HALVES)),
                dma((2, chips, HALVES)),
                dma((2, chips, HALVES)),
                dma((2, HALVES)),
                dma((2, 3)),
                dma((SLOTS, 2)),
                dma(()),
                dma((2, 2)),
                dma((2, 2)),
                dma((3 + d // TD,)),
                dma((2,)),
                pltpu.VMEM((2, d), F32),
            ],
            compiler_params=pltpu.CompilerParams(collective_id=0, has_side_effects=True, vmem_limit_bytes=67043328),
            name="layer",
        )(x.reshape(rows, d), gain_a, wq, wk, wv, wo, gain_m, w_gate, w_up, w_down)
        y = pl.pallas_call(
            functools.partial(_copy, rows, rows // 16),
            in_specs=[anywhere],
            out_specs=anywhere,
            out_shape=jax.ShapeDtypeStruct((rows, d), BF16),
            scratch_shapes=[pltpu.VMEM((16, rows // 16, d), BF16), dma((16,)), dma((16,))],
            name="copy_out",
        )(got)
        return y.reshape(x.shape)

    tokens, whole, columns, rows_of = P("dp", None, None), P(None), P(None, "tp"), P("tp", None)
    return jax.shard_map(
        step,
        mesh=mesh,
        in_specs=(tokens, whole, columns, columns, columns, rows_of, whole, columns, columns, rows_of),
        out_specs=tokens,
        check_vma=False,
    )
```

```python
import functools

import jax
import jax.numpy as jnp
from jax import lax
from jax.experimental import pallas as pl
from jax.experimental.pallas import tpu as pltpu
from jax.sharding import PartitionSpec as P

HEAD = 128
THETA = 10000
JOB = 256
TG = 256
TD = 512
SLOTS = 4
HALVES = 2
PIECES = 4
CHUNKS = (1, 1, 2, 2, 1, 1)
PLAN_FIRST = ((34099712, 1131010), (33554432, 332880))
PLAN_CHUNKS = (
    ((15, 8), (0, 0), ((17125478, 2688005), (20972802, 17449216)), 22),
    ((34, 21), (0, 0), ((5312597, 9769028), (1328137, 19022865)), 22),
    ((50, 37), (0, 0), ((39130457, 22103338), (43337046, 5525834)), 11),
    ((77, 63), (0, 0), ((5589668, 149), (18174633, 26633637)), 0),
    ((96, 96), (0, 0), ((22368896, 341), (0, 22106656)), 0),
    ((112, 106), (0, 0), ((18108544, 1), (1365, 17892610)), 99),
)
PLAN_TAIL = ((120, 119), 17, 130561)
HIDDEN = -1e30
F32, BF16 = jnp.float32, jnp.bfloat16


def _dot(a, b, ca=1, cb=0):
    return lax.dot_general(a, b, (((ca,), (cb,)), ((), ())), preferred_element_type=F32)


def _mod(a, n):
    return a & (n - 1)


def _over(a, n):
    return a >> (n.bit_length() - 1)


def _ds(start, size, unit=128):
    return pl.ds(pl.multiple_of(start, unit), size)


def _kernel(n, rows, length, d, heads, ff, *refs):
    (x, ga, wq, wk, wv, wo, gm, wg, wu, wd, G, town, tpar,
     tv_own, tv_par, xres, rrecv, rsend, fin, gout, hown, wbuf,
     exch_recv, agp_recv, rs_recv, rs_send, ag_recv, rs_last, ag_last, ag_sn, ag_sp, agl, tl, gsem, bsem, osem, psem, wsem, xsem, gains) = refs
    chips, half, blk = n // 2, JOB // 2, JOB // n
    nj = rows // JOB
    per = HALVES * chips
    half_plan = 13
    qw = heads * HEAD
    me = lax.axis_index("tp")
    chip, core = _over(me, 2), _mod(me, 2)
    step = 1 - 2 * core
    at = lambda c, k: _mod(c + chips, chips) * 2 + k
    nxt, prv, partner = at(chip + step, core), at(chip - step, core), at(chip, 1 - core)

    barrier = pltpu.get_barrier_semaphore()
    for other in (nxt, prv, partner):
        pl.semaphore_signal(barrier, inc=1, device_id={"tp": other}, device_id_type=pl.DeviceIdType.MESH)

    gains[0:1] = ga[...].astype(F32).reshape(1, d)
    gains[1:2] = gm[...].astype(F32).reshape(1, d)

    def remote(src, dst, send, recv, to):
        return pltpu.make_async_remote_copy(src_ref=src, dst_ref=dst, send_sem=send, recv_sem=recv, device_id={"tp": to},
                                            device_id_type=pl.DeviceIdType.MESH)

    local = pltpu.make_async_copy

    def event(e):
        alone = (e < 2 * per) | (e >= (nj - 1) * 2 * per)
        j = jnp.where(alone, _over(e, per), 2 * _over(e, 2 * per) + _mod(_over(e, HALVES), 2))
        return j, jnp.where(alone, _mod(_over(e, HALVES), chips), _mod(_over(e, 2 * HALVES), chips)), _mod(e, HALVES)

    def last_event(j):
        alone = (j < 2) | (j >= 2 * nj - 2)
        return per * j + per - 1 + jnp.where(alone | (_mod(j, 2) == 1), 0, per - HALVES)

    def loads(j):
        p = _mod(j, 2)
        mine = _ds(_mod(j, nj) * JOB + core * half + chip * blk, blk, blk)
        return (local(town.at[j], tv_own.at[p], tl.at[p, 0]), local(tpar.at[j], tv_par.at[p], tl.at[p, 1]),
                local(x.at[mine], xres.at[p], tl.at[p, 2]))

    def exchanged(j):
        return remote(tpar.at[j], tpar.at[j], psem.at[0, 0], exch_recv.at[j], partner)

    def tload(j):
        exchanged(j).wait_recv()
        for c in loads(j):
            c.start()

    def ring_sent(j, r):
        remote(rsend.at[_mod(j, 2), r], rrecv.at[_mod(j, 4), r], rs_send.at[_mod(j, 2), r], rs_recv.at[_mod(j, 4), r, 0], nxt).wait_send()

    def block(j, g):
        o = _mod(chip - step * g + chips * 2, chips)
        return _ds(j * JOB + core * half + o * blk, blk, blk)

    def to_partner(j, g, src):
        return remote(src, G.at[block(j, g)], ag_sp.at[_mod(j, 2), g], agp_recv.at[j], partner)

    def keep(j):
        return local(gout.at[_mod(j, 4)], G.at[block(j, 0)], agl.at[_mod(j, 2)])

    def ag_sent(j, g):
        whole = G.at[block(j, g)]
        to_partner(j, g, whole).wait_send()

        @pl.when(g < chips - 1)
        def _():
            remote(whole, whole, ag_sn.at[_mod(j, 2), g], ag_recv.at[_mod(j, 8), g, 0], nxt).wait_send()

    def finish(j):
        idx, p = _mod(j, nj), _mod(j, 2)

        @pl.when(j < nj)
        def _():
            h = (xres[p].astype(F32) + fin[...]).astype(BF16)
            hown[idx] = h
            wide = h.astype(F32)
            scale = lax.rsqrt(jnp.mean(wide * wide, -1, keepdims=True) + 1e-6)
            gout[_mod(j, 4)] = (wide * scale * gains[1:2]).astype(BF16)

        @pl.when(j >= nj)
        def _():
            gout[_mod(j, 4)] = (hown[idx].astype(F32) + fin[...]).astype(BF16)

    def rings(pieces, last):
        cw = d // pieces
        cols_of = lambda c: _ds(c * cw, cw)
        rs_at = (lambda j, r, c: rs_last.at[r, c]) if last else (lambda j, r, c: rs_recv.at[_mod(j, 4), r, c])
        ag_at = (lambda j, g, c: ag_last.at[g, c]) if last else (lambda j, g, c: ag_recv.at[_mod(j, 8), g, c])

        def ring(j, r, c):
            return remote(rsend.at[_mod(j, 2), r, :, cols_of(c)], rrecv.at[_mod(j, 4), r, :, cols_of(c)], rs_send.at[_mod(j, 2), r],
                          rs_at(j, r, c), nxt)

        def rs_do(j, r, c, avail=None):
            p = _mod(j, 2)
            o = _mod(chip + step * (chips - 1 - r) + chips * 2, chips)
            there, cols = _ds(o * blk, blk, blk), cols_of(c)

            @pl.when((r == 0) & (c == 0))
            def _():
                for copy in loads(j):
                    copy.wait()

            def both():
                return tv_own[p, there, cols] + tv_par[p, there, cols].astype(F32)

            def send(value):
                @pl.when((j >= 2) & (c == 0))
                def _():
                    ring_sent(j - 2, r)

                rsend[p, r, :, cols] = value.astype(BF16)
                ring(j, r, c).start()

            @pl.when(r == 0)
            def _():
                send(both())

            @pl.when(r > 0)
            def _():
                ring(j, r - 1, c).wait_recv()

            @pl.when((r > 0) & (r < chips - 1))
            def _():
                send(both() + rrecv[_mod(j, 4), r - 1, :, cols].astype(F32))

            if last:
                @pl.when(r == chips - 1)
                def _():
                    total = both() + rrecv[_mod(j, 4), r - 1, :, cols].astype(F32)
                    gout[_mod(j, 4), :, cols] = (hown[_mod(j, nj), :, cols].astype(F32) + total).astype(BF16)
            else:
                @pl.when(r == chips - 1)
                def _():
                    fin[:, cols] = both() + rrecv[_mod(j, 4), r - 1, :, cols].astype(F32)

                @pl.when((r == chips - 1) & (c == pieces - 1))
                def _():
                    finish(j)

                    @pl.when(j + 2 <= avail)
                    def _():
                        tload(j + 2)

        def to_next(j, g, c, src):
            return remote(src, G.at[block(j, g), cols_of(c)], ag_sn.at[_mod(j, 2), g], ag_at(j, g, c), nxt)

        def ag_do(j, g, c):
            here = G.at[block(j, g), cols_of(c)]

            @pl.when((j >= 2) & (c == 0))
            def _():
                ag_sent(j - 2, g)

            @pl.when(g == 0)
            def _():
                to_next(j, g, c, gout.at[_mod(j, 4), :, cols_of(c)]).start()

                @pl.when(c == pieces - 1)
                def _():
                    to_partner(j, g, gout.at[_mod(j, 4)]).start()
                    keep(j).start()

            @pl.when(g > 0)
            def _():
                to_next(j, g - 1, c, here).wait_recv()

                @pl.when(g < chips - 1)
                def _():
                    to_next(j, g, c, here).start()

                @pl.when(c == pieces - 1)
                def _():
                    to_partner(j, g, G.at[block(j, g)]).start()

                    @pl.when(g == chips - 1)
                    def _():
                        keep(j).wait()

        return rs_do, ag_do

    rs_do, ag_do = rings(HALVES, False)
    rs_event = lambda e, avail: rs_do(*event(e), avail)
    ag_event = lambda e: ag_do(*event(e))

    def gathered(j):
        there = G.at[_ds(j * JOB, half, half)]
        remote(there, there, ag_sp.at[0, 0], agp_recv.at[j], partner).wait_recv()

    def pump(plan, t, at_, avail):
        (a0, a1), (b0, b1) = plan
        u = 2 * jnp.where(t < half_plan, t, t - half_plan)
        a = lax.shift_right_logical(jnp.where(t < half_plan, a0, a1), u) & 3
        b = lax.shift_right_logical(jnp.where(t < half_plan, b0, b1), u) & 3
        r, g = at_
        lax.fori_loop(r, r + a, lambda e, _: rs_event(e, avail), None)
        lax.fori_loop(g, g + b, lambda e, _: ag_event(e), None)
        return r + a, g + b

    def catch_up(j, at_):
        @pl.when((j < 2) | (last_event(j - 2) < at_[0]))
        def _():
            tload(j)

    n1, n2 = ff // TG, d // TD
    ticks = n1 + n2
    slot_of = lambda k, t: _mod(k * ticks + 3 + t, SLOTS)

    def g_copies(k, t):
        col, s = _ds(t * TG, TG), slot_of(k, t)
        return (local(wg.at[:, col], wbuf.at[s, :, pl.ds(0, TG)], gsem.at[s, 0]),
                local(wu.at[:, col], wbuf.at[s, :, pl.ds(TG, TG)], gsem.at[s, 1]))

    def d_copy(k, t):
        s = slot_of(k, t)
        return local(wd.at[:, _ds((t - n1) * TD, TD)], wbuf.at[s, pl.ds(0, ff)], gsem.at[s, 0])

    def fetch(k, t):
        for c in g_copies(k, t):
            c.start()

    def first(xb, ab, qb, kb, vb, seen, own_st, par_st, cos, sin):
        nh = rows // JOB
        up = length // JOB
        wcopies = [local(wq, wbuf.at[0], wsem.at[0]), local(wk, wbuf.at[1, :, pl.ds(0, HEAD)], wsem.at[1]),
                   local(wv, wbuf.at[1, :, pl.ds(HEAD, HEAD)], wsem.at[2])]
        wcopies += [local(wo.at[:, pl.ds(t * TD, TD)], wbuf.at[2, pl.ds(t * qw, qw)], wsem.at[3 + t]) for t in range(n2)]
        x_copy = lambda h: local(x.at[_ds(h * JOB, JOB, JOB)], xb.at[_mod(h, 2)], xsem.at[_mod(h, 2)])
        x_copy(0).start()
        for c in wcopies[:3]:
            c.start()
        lane = lax.broadcasted_iota(jnp.int32, (16, HEAD), 1)
        row = lax.broadcasted_iota(jnp.int32, (16, HEAD), 0).astype(F32)
        power = jnp.exp((lane % (HEAD // 2)).astype(F32) * (-2.0 / HEAD) * jnp.log(jnp.float32(THETA)))
        sign = jnp.where(lane < HEAD // 2, -1.0, 1.0)
        cf, sf = jnp.cos(row * power), jnp.sin(row * power)
        for a in range(0, length, 256):
            cc, sc = jnp.cos((16 * row + a) * power), jnp.sin((16 * row + a) * power)
            for i in range(16):
                at_ = slice(a + 16 * i, a + 16 * (i + 1))
                ci, si = cc[i : i + 1], sc[i : i + 1]
                cos[at_, :] = ci * cf - si * sf
                sin[at_, :] = sign * (si * cf + ci * sf)

        def out(h):
            return (local(own_st, town.at[h], osem.at[0, 0]), remote(par_st, tpar.at[h], psem.at[0, 0], exch_recv.at[h], partner))

        def normed(h):
            for a in range(0, JOB, 16):
                rows_ = slice(a, a + 16)
                wide = xb[_mod(h, 2), rows_, :].astype(F32)
                scale = lax.rsqrt(jnp.mean(wide * wide, -1, keepdims=True) + 1e-6)
                ab[_mod(h, 2), rows_, :] = (xb[_mod(h, 2), rows_, :].astype(F32) * scale * gains[0:1]).astype(BF16)

        x_copy(0).wait()
        normed(0)
        x_copy(1).start()
        for c in wcopies[:3]:
            c.wait()
        for c in wcopies[3:]:
            c.start()

        pl.semaphore_wait(barrier, 3)

        def body(h, at_):
            at_seq = (_mod(h, up)) * JOB

            @pl.when(h + 1 < nh)
            def _():
                x_copy(h + 1).wait()

            here = _ds(at_seq, JOB, JOB)
            cosv, sinv = cos[here, :], sin[here, :]

            def turned(t):
                t = t.astype(BF16).astype(F32)
                return (t * cosv + pltpu.roll(t, HEAD // 2, 1) * sinv).astype(BF16)

            queries = _dot(ab[_mod(h, 2)], wbuf[0])
            others = _dot(ab[_mod(h, 2)], wbuf[1, :, : 2 * HEAD])
            normed(h + 1)
            kb[here, :] = turned(others[:, :HEAD])
            vb[here, :] = others[:, HEAD:].astype(BF16)
            for m in range(heads):
                qb[:, m * HEAD : (m + 1) * HEAD] = turned(queries[:, m * HEAD : (m + 1) * HEAD])

            @pl.when(h + 2 < nh)
            def _():
                x_copy(h + 2).start()

            @pl.when(h == nh - 1)
            def _():
                fetch(0, 1)
                fetch(0, 2)

            @pl.when(h == 0)
            def _():
                for c in wcopies[3:]:
                    c.wait()

            @pl.when(h == 3)
            def _():
                fetch(0, 0)

            at_ = pump(PLAN_FIRST, 3 * h, at_, h - 2)

            def attend(keys):
                ok = (keys - JOB + lax.broadcasted_iota(jnp.int32, (JOB, keys), 0)) >= lax.broadcasted_iota(jnp.int32, (JOB, keys), 1)
                for m in range(heads):
                    s = _dot(qb[:, m * HEAD : (m + 1) * HEAD], kb[:keys], 1, 1) * HEAD**-0.5
                    s = jnp.where(ok, s, HIDDEN)
                    w = jnp.exp(s - s.max(-1, keepdims=True))
                    total = w.sum(-1, keepdims=True)
                    seen[:, m * HEAD : (m + 1) * HEAD] = (_dot(w.astype(BF16), vb[:keys]) / total).astype(BF16)

            for part in range(up):
                @pl.when(_mod(h, up) == part)
                def _():
                    attend((part + 1) * JOB)

            @pl.when(h >= 1)
            def _():
                own, par = out(h - 1)
                own.wait()
                par.wait_send()
                catch_up(h - 1, at_)

            at_ = pump(PLAN_FIRST, 3 * h + 1, at_, h - 1)

            for t in range(n2):
                cols = slice(t * TD, (t + 1) * TD)
                val = _dot(seen[...], wbuf[2, t * qw : (t + 1) * qw])
                v0, v1 = val[:half], val[half:]
                own_st[:, cols] = jnp.where(core == 0, v0, v1)
                par_st[:, cols] = jnp.where(core == 0, v1, v0).astype(BF16)
            for c in out(h):
                c.start()
            return pump(PLAN_FIRST, 3 * h + 2, at_, h - 1)

        lax.fori_loop(0, nh, body, (jnp.int32(0), jnp.int32(0)))
        own, par = out(nh - 1)
        own.wait()
        par.wait_send()
        catch_up(nh - 1, PLAN_CHUNKS[0][0])

    pl.run_scoped(first, pltpu.VMEM((2, JOB, d), BF16), pltpu.VMEM((2, JOB, d), BF16), pltpu.VMEM((JOB, qw), BF16), pltpu.VMEM((length, HEAD), BF16),
                  pltpu.VMEM((length, HEAD), BF16), pltpu.VMEM((JOB, qw), BF16), pltpu.VMEM((half, d), F32), pltpu.VMEM((half, d), BF16),
                  pltpu.VMEM((length, HEAD), F32), pltpu.VMEM((length, HEAD), F32))


    def second(bb, hid, ost, pst):
        def b_copy(first_job, jobs, s):
            return local(G.at[_ds(first_job * JOB, jobs * JOB, JOB)], bb.at[s, pl.ds(0, jobs * JOB)], bsem)

        def outs(first_job, t, q):
            col = _ds(t * TD, TD)
            job = nj + first_job + q
            return (local(ost.at[_mod(t, 2), q], town.at[job, :, col], osem.at[_mod(t, 2), q]),
                    remote(pst.at[_mod(t, 2), q], tpar.at[job, :, col], psem.at[_mod(t, 2), q], exch_recv.at[job], partner))

        def settle(first_job, t, q):
            own, par = outs(first_job, t, q)
            own.wait()
            par.wait_send()

        def chunk(k, first_job, jobs, at_, plan, before, load):
            m = jobs * JOB
            s = _mod(k, 2)
            avail = nj + first_job - 1

            def g_tile(t, at_):
                @pl.when(t < n1 - (SLOTS - 1))
                def _():
                    fetch(k, t + SLOTS - 1)

                @pl.when(t >= n1 - (SLOTS - 1))
                def _():
                    d_copy(k, t + SLOTS - 1).start()

                @pl.when(t == 1)
                def _():
                    for q in range(2):
                        @pl.when(q < before)
                        def _():
                            for u in (n2 - 2, n2 - 1):
                                settle(first_job - before, u, q)

                    for q in (2, 1):
                        @pl.when(q <= before)
                        def _():
                            catch_up(nj + first_job - q, at_)

                for c in g_copies(k, t):
                    c.wait()
                r = _dot(bb[s, :m], wbuf[slot_of(k, t)])
                gate, upv = r[:, :TG], r[:, TG:]
                hid[:m, _ds(t * TG, TG)] = (jax.nn.silu(gate) * upv).astype(BF16)
                at_ = pump(plan, t, at_, jnp.where(t >= 1, avail, avail - before))
                load(t)
                return at_

            at_ = lax.fori_loop(0, n1, g_tile, at_)

            def d_tile(t, at_):
                @pl.when(t < n2 - (SLOTS - 1))
                def _():
                    d_copy(k, n1 + t + SLOTS - 1).start()

                @pl.when((t >= n2 - (SLOTS - 1)) & (k < len(CHUNKS) - 1))
                def _():
                    fetch(k + 1, t + SLOTS - 1 - n2)

                d_copy(k, n1 + t).wait()

                @pl.when(t >= 2)
                def _():
                    for q in range(jobs):
                        settle(first_job, t - 2, q)

                val = _dot(hid[:m], wbuf[slot_of(k, n1 + t), :ff])
                for q in range(jobs):
                    v0, v1 = val[q * JOB : q * JOB + half], val[q * JOB + half : (q + 1) * JOB]
                    ost[_mod(t, 2), q] = jnp.where(core == 0, v0, v1)
                    pst[_mod(t, 2), q] = jnp.where(core == 0, v1, v0).astype(BF16)
                    for c in outs(first_job, t, q):
                        c.start()
                at_ = pump(plan, n1 + t, at_, avail)
                load(n1 + t)
                return at_

            lax.fori_loop(0, n2, d_tile, at_)

        def have(first_job, jobs, s):
            for q in range(jobs):
                gathered(first_job + q)
            b_copy(first_job, jobs, s).start()

        def run(lo, hi):
            jobs = CHUNKS[lo]
            ks = range(lo, hi)

            def body(k, _):
                def pick(f):
                    value = f(lo)
                    for i in ks[1:]:
                        value = jnp.where(k == i, f(i), value) if f(i) != f(lo) else value
                    return jnp.int32(value)

                first_job = pick(lambda i: sum(CHUNKS[:i]))
                r, g = (pick(lambda i: PLAN_CHUNKS[i][0][q]) for q in (0, 1))
                ahead = [pick(lambda i: PLAN_CHUNKS[i][1][q]) for q in (0, 1)]
                plan = [[pick(lambda i: PLAN_CHUNKS[i][2][q][u]) for u in (0, 1)] for q in (0, 1)]
                before = pick(lambda i: CHUNKS[i - 1] if i else 0)
                after = pick(lambda i: CHUNKS[i + 1] if i + 1 < len(CHUNKS) else 0)
                when = pick(lambda i: PLAN_CHUNKS[i][3])

                lax.fori_loop(r, r + ahead[0], lambda e, _: rs_event(e, nj + first_job - before - 1), None)
                lax.fori_loop(g, g + ahead[1], lambda e, _: ag_event(e), None)

                @pl.when(pick(lambda i: int(i == 0 or PLAN_CHUNKS[i - 1][3] >= ticks)) == 1)
                def _():
                    have(first_job, jobs, _mod(k, 2))

                b_copy(0, jobs, 0).wait()

                def load(t):
                    @pl.when(t == when)
                    def _():
                        for q in (1, 2):
                            @pl.when(after == q)
                            def _():
                                have(first_job + jobs, q, _mod(k + 1, 2))

                chunk(k, first_job, jobs, (r + ahead[0], g + ahead[1]), plan, before, load)

            lax.fori_loop(lo, hi, body, None)

        lo = 0
        for hi in range(1, len(CHUNKS) + 1):
            if hi == len(CHUNKS) or CHUNKS[hi] != CHUNKS[lo]:
                run(lo, hi)
                lo = hi
        for q in range(CHUNKS[-1]):
            for u in (n2 - 2, n2 - 1):
                settle(nj - CHUNKS[-1], u, q)

    pl.run_scoped(second, pltpu.VMEM((2, 2 * JOB, d), BF16), pltpu.VMEM((2 * JOB, ff), BF16),
                  pltpu.VMEM((2, 2, half, TD), F32), pltpu.VMEM((2, 2, half, TD), BF16))

    done = PLAN_TAIL[0]
    last = 2 * nj - 1
    catch_up(last, done)
    lax.fori_loop(done[1], per * last, lambda e, _: ag_event(e), None)
    rs_last_do, ag_last_do = rings(PIECES, True)
    both_from = (chips - 1) * PIECES

    def tail(t, _):
        u = t - both_from
        mixed = (u >= 0) & (u < 2 * PIECES)
        gather = (mixed & (_mod(u, 2) == 1)) | (u >= 2 * PIECES)
        at_ = jnp.where(mixed, _over(u, 2), u - PIECES)

        @pl.when(jnp.logical_not(gather))
        def _():
            i = jnp.where(mixed, both_from + at_, t)
            rs_last_do(jnp.int32(last), _over(i, PIECES), _mod(i, PIECES))

        @pl.when(gather)
        def _():
            ag_last_do(jnp.int32(last), _over(at_, PIECES), _mod(at_, PIECES))

    lax.fori_loop(0, 2 * chips * PIECES, tail, None)
    for j in (2 * nj - 2, 2 * nj - 1):
        for r in range(chips - 1):
            ring_sent(j, r)
        for g in range(chips):
            ag_sent(jnp.int32(j), jnp.int32(g))

    def all_here(j, _):
        gathered(j)

    lax.fori_loop(nj, 2 * nj, all_here, None)


def _copy(start, size, src, dst, buf, get, put):
    n = buf.shape[0]
    ins = [pltpu.make_async_copy(src.at[pl.ds(start + i * size, size)], buf.at[i], get.at[i]) for i in range(n)]
    outs = [pltpu.make_async_copy(buf.at[i], dst.at[pl.ds(i * size, size)], put.at[i]) for i in range(n)]
    for c in ins:
        c.start()
    for i in range(n):
        ins[i].wait()
        outs[i].start()
    for c in outs:
        c.wait()


def solution(mesh):
    n = mesh.shape["tp"]
    chips = n // 2

    def step(x, gain_a, wq, wk, wv, wo, gain_m, w_gate, w_up, w_down):
        batch, length, d = x.shape
        rows, heads, ff = batch * length, wq.shape[1] // HEAD, w_gate.shape[1]
        nj, half, blk = rows // JOB, JOB // 2, JOB // n
        dma, anywhere, vmem = pltpu.SemaphoreType.DMA, pl.BlockSpec(memory_space=pl.ANY), pl.BlockSpec(memory_space=pltpu.VMEM)
        got, _, _ = pl.pallas_call(
            functools.partial(_kernel, n, rows, length, d, heads, ff),
            in_specs=[anywhere, vmem, anywhere, anywhere, anywhere, anywhere, vmem, anywhere, anywhere, anywhere],
            out_specs=[anywhere] * 3,
            out_shape=[jax.ShapeDtypeStruct((2 * rows, d), BF16), jax.ShapeDtypeStruct((2 * nj, half, d), F32),
                       jax.ShapeDtypeStruct((2 * nj, half, d), BF16)],
            scratch_shapes=[
                pltpu.VMEM((2, half, d), F32),
                pltpu.VMEM((2, half, d), BF16),
                pltpu.VMEM((2, blk, d), BF16),
                pltpu.VMEM((4, chips - 1, blk, d), BF16),
                pltpu.VMEM((2, chips - 1, blk, d), BF16),
                pltpu.VMEM((blk, d), F32),
                pltpu.VMEM((4, blk, d), BF16),
                pltpu.VMEM((nj, blk, d), BF16),
                pltpu.VMEM((SLOTS, d, 2 * TG), BF16),
                dma((2 * nj,)),
                dma((2 * nj,)),
                dma((4, chips - 1, HALVES)),
                dma((2, chips - 1)),
                dma((8, chips - 1, HALVES)),
                dma((chips - 1, PIECES)),
                dma((chips - 1, PIECES)),
                dma((2, chips)),
                dma((2, chips)),
                dma((2,)),
                dma((2, 3)),
                dma((SLOTS, 2)),
                dma(()),
                dma((2, 2)),
                dma((2, 2)),
                dma((3 + d // TD,)),
                dma((2,)),
                pltpu.VMEM((2, d), F32),
            ],
            compiler_params=pltpu.CompilerParams(collective_id=0, has_side_effects=True, vmem_limit_bytes=67043328),
            name="layer",
        )(x.reshape(rows, d), gain_a, wq, wk, wv, wo, gain_m, w_gate, w_up, w_down)
        y = pl.pallas_call(
            functools.partial(_copy, rows, rows // 16),
            in_specs=[anywhere],
            out_specs=anywhere,
            out_shape=jax.ShapeDtypeStruct((rows, d), BF16),
            scratch_shapes=[pltpu.VMEM((16, rows // 16, d), BF16), dma((16,)), dma((16,))],
            name="copy_out",
        )(got)
        return y.reshape(x.shape)

    tokens, whole, columns, rows_of = P("dp", None, None), P(None), P(None, "tp"), P("tp", None)
    return jax.shard_map(
        step,
        mesh=mesh,
        in_specs=(tokens, whole, columns, columns, columns, rows_of, whole, columns, columns, rows_of),
        out_specs=tokens,
        check_vma=False,
    )
```

```python
import functools

import jax
import jax.numpy as jnp
from jax import lax
from jax.experimental import pallas as pl
from jax.experimental.pallas import tpu as pltpu
from jax.sharding import PartitionSpec as P

HEAD = 128
THETA = 10000
JOB = 256
TG = 256
TD = 512
SLOTS = 4
HALVES = 2
PIECES = 4
CHUNKS = (1, 1, 2, 2, 1, 1)
PLAN_FIRST = ((34949120, 1131010), (33554432, 332880))
PLAN_CHUNKS = (
    ((15, 8), (0, 0), ((69653, 17317905), (5243202, 17056832)), 20),
    ((26, 19), (0, 0), ((263172, 2098177), (16793664, 1179712)), 23),
    ((33, 26), (0, 0), ((25445397, 4260929), (23138565, 1065232)), 11),
    ((47, 39), (0, 0), ((1118296, 17), (17056790, 18105624)), 0),
    ((56, 56), (0, 0), ((17055872, 4164), (0, 17043520)), 0),
    ((64, 60), (0, 0), ((8409216, 20), (1052740, 17895456)), 99),
)
PLAN_TAIL = ((72, 70), 18, 261129)
HIDDEN = -1e30
F32, BF16 = jnp.float32, jnp.bfloat16


def _dot(a, b, ca=1, cb=0):
    return lax.dot_general(a, b, (((ca,), (cb,)), ((), ())), preferred_element_type=F32)


def _mod(a, n):
    return a & (n - 1)


def _over(a, n):
    return a >> (n.bit_length() - 1)


def _ds(start, size, unit=128):
    return pl.ds(pl.multiple_of(start, unit), size)


def _kernel(n, rows, length, d, heads, ff, *refs):
    (x, ga, wq, wk, wv, wo, gm, wg, wu, wd, G, town, tpar,
     tv_own, tv_par, xres, rrecv, rsend, fin, gout, hown, wbuf,
     exch_recv, agp_recv, rs_recv, rs_send, ag_recv, rs_last, ag_last, ag_sn, ag_sp, agl, tl, gsem, bsem, osem, psem, wsem, xsem, gains) = refs
    chips, half, blk = n // 2, JOB // 2, JOB // n
    nj = rows // JOB
    per = HALVES * chips
    half_plan = 13
    qw = heads * HEAD
    me = lax.axis_index("tp")
    chip, core = _over(me, 2), _mod(me, 2)
    step = 1 - 2 * core
    at = lambda c, k: _mod(c + chips, chips) * 2 + k
    nxt, prv, partner = at(chip + step, core), at(chip - step, core), at(chip, 1 - core)

    barrier = pltpu.get_barrier_semaphore()
    for other in (nxt, prv, partner):
        pl.semaphore_signal(barrier, inc=1, device_id={"tp": other}, device_id_type=pl.DeviceIdType.MESH)

    gains[0:1] = ga[...].astype(F32).reshape(1, d)
    gains[1:2] = gm[...].astype(F32).reshape(1, d)

    def remote(src, dst, send, recv, to):
        return pltpu.make_async_remote_copy(src_ref=src, dst_ref=dst, send_sem=send, recv_sem=recv, device_id={"tp": to},
                                            device_id_type=pl.DeviceIdType.MESH)

    local = pltpu.make_async_copy

    early = 2 * per
    late = early + (nj - 2) * per
    ended = late + per

    def alone(e):
        return (e < early) | (e >= late)

    def event(e):
        single = jnp.where(e < early, _over(e, per), 2 * nj - 2)
        return jnp.where(alone(e), single, 2 + 2 * _over(e - early, per) + _mod(e, 2)), _mod(_over(e, 2), chips), _mod(e, 2)

    def last_event(j):
        paired = early + per * (_over(j, 2) - 1) + per - 2 + _mod(j, 2)
        return jnp.where(j < 2, per * j + per - 1, jnp.where(j < 2 * nj - 2, paired, late + per - 1))

    def loads(j):
        p = _mod(j, 2)
        mine = _ds(_mod(j, nj) * JOB + core * half + chip * blk, blk, blk)
        return (local(town.at[j], tv_own.at[p], tl.at[p, 0]), local(tpar.at[j], tv_par.at[p], tl.at[p, 1]),
                local(x.at[mine], xres.at[p], tl.at[p, 2]))

    def exchanged(j):
        return remote(tpar.at[j], tpar.at[j], psem.at[0, 0], exch_recv.at[j], partner)

    def tload(j):
        exchanged(j).wait_recv()
        for c in loads(j):
            c.start()

    def ring_sent(j, r):
        remote(rsend.at[_mod(j, 2), r], rrecv.at[_mod(j, 4), r], rs_send.at[_mod(j, 2), r], rs_recv.at[_mod(j, 4), r, 0], nxt).wait_send()

    def block(j, g):
        o = _mod(chip - step * g + chips * 2, chips)
        return _ds(j * JOB + core * half + o * blk, blk, blk)

    def to_partner(j, g, src):
        return remote(src, G.at[block(j, g)], ag_sp.at[_mod(j, 2), g], agp_recv.at[j], partner)

    def keep(j):
        return local(gout.at[_mod(j, 4)], G.at[block(j, 0)], agl.at[_mod(j, 2)])

    def ag_sent(j, g):
        whole = G.at[block(j, g)]
        to_partner(j, g, whole).wait_send()

        @pl.when(g < chips - 1)
        def _():
            remote(whole, whole, ag_sn.at[_mod(j, 2), g], ag_recv.at[_mod(j, 8), g, 0], nxt).wait_send()

    def finish(j):
        idx, p = _mod(j, nj), _mod(j, 2)

        @pl.when(j < nj)
        def _():
            h = (xres[p].astype(F32) + fin[...]).astype(BF16)
            hown[idx] = h
            wide = h.astype(F32)
            scale = lax.rsqrt(jnp.mean(wide * wide, -1, keepdims=True) + 1e-6)
            gout[_mod(j, 4)] = (wide * scale * gains[1:2]).astype(BF16)

        @pl.when(j >= nj)
        def _():
            gout[_mod(j, 4)] = (hown[idx].astype(F32) + fin[...]).astype(BF16)

    def rings(pieces, last):
        cw = d // pieces
        cols_of = lambda c: pl.ds(0, d) if pieces == 1 else _ds(c * cw, cw)
        rs_at = (lambda j, r, c: rs_last.at[r, c]) if last else (lambda j, r, c: rs_recv.at[_mod(j, 4), r, c])
        ag_at = (lambda j, g, c: ag_last.at[g, c]) if last else (lambda j, g, c: ag_recv.at[_mod(j, 8), g, c])

        def ring(j, r, c):
            return remote(rsend.at[_mod(j, 2), r, :, cols_of(c)], rrecv.at[_mod(j, 4), r, :, cols_of(c)], rs_send.at[_mod(j, 2), r],
                          rs_at(j, r, c), nxt)

        def rs_do(j, r, c, avail=None):
            p = _mod(j, 2)
            o = _mod(chip + step * (chips - 1 - r) + chips * 2, chips)
            there = _ds(o * blk, blk, blk)

            @pl.when((r == 0) & (c == 0))
            def _():
                for copy in loads(j):
                    copy.wait()

            def both(cols):
                return tv_own[p, there, cols] + tv_par[p, there, cols].astype(F32)

            def all_(cols):
                return both(cols) + rrecv[_mod(j, 4), r - 1, :, cols].astype(F32)

            def send(total):
                @pl.when((j >= 2) & (c == 0))
                def _():
                    ring_sent(j - 2, r)

                rsend[p, r, :, cols_of(c)] = total(cols_of(c)).astype(BF16)
                ring(j, r, c).start()

            @pl.when(r == 0)
            def _():
                send(both)

            @pl.when(r > 0)
            def _():
                ring(j, r - 1, c).wait_recv()

            @pl.when((r > 0) & (r < chips - 1))
            def _():
                send(all_)

            @pl.when(r == chips - 1)
            def _():
                cols = cols_of(c)
                if last:
                    gout[_mod(j, 4), :, cols] = (hown[_mod(j, nj), :, cols].astype(F32) + all_(cols)).astype(BF16)
                else:
                    fin[:, cols] = all_(cols)

            if not last:
                @pl.when((r == chips - 1) & (c == pieces - 1))
                def _():
                    finish(j)

                    @pl.when(j + 2 <= avail)
                    def _():
                        tload(j + 2)

        def to_next(j, g, c, src):
            return remote(src, G.at[block(j, g), cols_of(c)], ag_sn.at[_mod(j, 2), g], ag_at(j, g, c), nxt)

        def ag_do(j, g, c):
            here = G.at[block(j, g), cols_of(c)]

            @pl.when((j >= 2) & (c == 0))
            def _():
                ag_sent(j - 2, g)

            @pl.when(g == 0)
            def _():
                to_next(j, g, c, gout.at[_mod(j, 4), :, cols_of(c)]).start()

                @pl.when(c == pieces - 1)
                def _():
                    to_partner(j, g, gout.at[_mod(j, 4)]).start()
                    keep(j).start()

            @pl.when(g > 0)
            def _():
                to_next(j, g - 1, c, here).wait_recv()

                @pl.when(g < chips - 1)
                def _():
                    to_next(j, g, c, here).start()

                @pl.when(c == pieces - 1)
                def _():
                    to_partner(j, g, G.at[block(j, g)]).start()

                    @pl.when(g == chips - 1)
                    def _():
                        keep(j).wait()

        return rs_do, ag_do

    rs_piece, ag_piece = rings(HALVES, False)
    rs_whole, ag_whole = rings(1, False)

    def rs_event(e, avail):
        j, r, which = event(e)

        @pl.when(alone(e))
        def _():
            rs_piece(j, r, which, avail)

        @pl.when(jnp.logical_not(alone(e)))
        def _():
            rs_whole(j, r, 0, avail)

    def ag_event(e):
        j, g, which = event(e)

        @pl.when(alone(e))
        def _():
            ag_piece(j, g, which)

        @pl.when(jnp.logical_not(alone(e)))
        def _():
            ag_whole(j, g, 0)

    def gathered(j):
        there = G.at[_ds(j * JOB, half, half)]
        remote(there, there, ag_sp.at[0, 0], agp_recv.at[j], partner).wait_recv()

    def pump(plan, t, at_, avail):
        (a0, a1), (b0, b1) = plan
        u = 2 * jnp.where(t < half_plan, t, t - half_plan)
        a = lax.shift_right_logical(jnp.where(t < half_plan, a0, a1), u) & 3
        b = lax.shift_right_logical(jnp.where(t < half_plan, b0, b1), u) & 3
        r, g = at_
        lax.fori_loop(r, r + a, lambda e, _: rs_event(e, avail), None)
        lax.fori_loop(g, g + b, lambda e, _: ag_event(e), None)
        return r + a, g + b

    def catch_up(j, at_):
        @pl.when((j < 2) | (last_event(j - 2) < at_[0]))
        def _():
            tload(j)

    n1, n2 = ff // TG, d // TD
    ticks = n1 + n2
    slot_of = lambda k, t: _mod(k * ticks + 3 + t, SLOTS)

    def g_copies(k, t):
        col, s = _ds(t * TG, TG), slot_of(k, t)
        return (local(wg.at[:, col], wbuf.at[s, :, pl.ds(0, TG)], gsem.at[s, 0]),
                local(wu.at[:, col], wbuf.at[s, :, pl.ds(TG, TG)], gsem.at[s, 1]))

    def d_copy(k, t):
        s = slot_of(k, t)
        return local(wd.at[:, _ds((t - n1) * TD, TD)], wbuf.at[s, pl.ds(0, ff)], gsem.at[s, 0])

    def fetch(k, t):
        for c in g_copies(k, t):
            c.start()

    def first(xb, ab, qb, kb, vb, seen, own_st, par_st, cos, sin):
        nh = rows // JOB
        up = length // JOB
        wcopies = [local(wq, wbuf.at[0], wsem.at[0]), local(wk, wbuf.at[1, :, pl.ds(0, HEAD)], wsem.at[1]),
                   local(wv, wbuf.at[1, :, pl.ds(HEAD, HEAD)], wsem.at[2])]
        wcopies += [local(wo.at[:, pl.ds(t * TD, TD)], wbuf.at[2, pl.ds(t * qw, qw)], wsem.at[3 + t]) for t in range(n2)]
        x_copy = lambda h: local(x.at[_ds(h * JOB, JOB, JOB)], xb.at[_mod(h, 2)], xsem.at[_mod(h, 2)])
        x_copy(0).start()
        for c in wcopies[:3]:
            c.start()
        lane = lax.broadcasted_iota(jnp.int32, (16, HEAD), 1)
        row = lax.broadcasted_iota(jnp.int32, (16, HEAD), 0).astype(F32)
        power = jnp.exp((lane % (HEAD // 2)).astype(F32) * (-2.0 / HEAD) * jnp.log(jnp.float32(THETA)))
        sign = jnp.where(lane < HEAD // 2, -1.0, 1.0)
        cf, sf = jnp.cos(row * power), jnp.sin(row * power)
        for a in range(0, length, 256):
            cc, sc = jnp.cos((16 * row + a) * power), jnp.sin((16 * row + a) * power)
            for i in range(16):
                at_ = slice(a + 16 * i, a + 16 * (i + 1))
                ci, si = cc[i : i + 1], sc[i : i + 1]
                cos[at_, :] = ci * cf - si * sf
                sin[at_, :] = sign * (si * cf + ci * sf)

        def out(h):
            return (local(own_st, town.at[h], osem.at[0, 0]), remote(par_st, tpar.at[h], psem.at[0, 0], exch_recv.at[h], partner))

        def normed(h):
            for a in range(0, JOB, 16):
                rows_ = slice(a, a + 16)
                wide = xb[_mod(h, 2), rows_, :].astype(F32)
                scale = lax.rsqrt(jnp.mean(wide * wide, -1, keepdims=True) + 1e-6)
                ab[_mod(h, 2), rows_, :] = (xb[_mod(h, 2), rows_, :].astype(F32) * scale * gains[0:1]).astype(BF16)

        x_copy(0).wait()
        normed(0)
        x_copy(1).start()
        for c in wcopies[:3]:
            c.wait()
        for c in wcopies[3:]:
            c.start()

        pl.semaphore_wait(barrier, 3)

        def body(h, at_):
            at_seq = (_mod(h, up)) * JOB

            @pl.when(h + 1 < nh)
            def _():
                x_copy(h + 1).wait()

            here = _ds(at_seq, JOB, JOB)
            cosv, sinv = cos[here, :], sin[here, :]

            def turned(t):
                t = t.astype(BF16).astype(F32)
                return (t * cosv + pltpu.roll(t, HEAD // 2, 1) * sinv).astype(BF16)

            queries = _dot(ab[_mod(h, 2)], wbuf[0])
            others = _dot(ab[_mod(h, 2)], wbuf[1, :, : 2 * HEAD])
            normed(h + 1)
            kb[here, :] = turned(others[:, :HEAD])
            vb[here, :] = others[:, HEAD:].astype(BF16)
            for m in range(heads):
                qb[:, m * HEAD : (m + 1) * HEAD] = turned(queries[:, m * HEAD : (m + 1) * HEAD])

            @pl.when(h + 2 < nh)
            def _():
                x_copy(h + 2).start()

            @pl.when(h == nh - 1)
            def _():
                fetch(0, 1)
                fetch(0, 2)

            @pl.when(h == 0)
            def _():
                for c in wcopies[3:]:
                    c.wait()

            @pl.when(h == 3)
            def _():
                fetch(0, 0)

            at_ = pump(PLAN_FIRST, 3 * h, at_, h - 2)

            def attend(keys):
                ok = (keys - JOB + lax.broadcasted_iota(jnp.int32, (JOB, keys), 0)) >= lax.broadcasted_iota(jnp.int32, (JOB, keys), 1)
                for m in range(heads):
                    s = _dot(qb[:, m * HEAD : (m + 1) * HEAD], kb[:keys], 1, 1) * HEAD**-0.5
                    s = jnp.where(ok, s, HIDDEN)
                    w = jnp.exp(s - s.max(-1, keepdims=True))
                    total = w.sum(-1, keepdims=True)
                    seen[:, m * HEAD : (m + 1) * HEAD] = (_dot(w.astype(BF16), vb[:keys]) / total).astype(BF16)

            for part in range(up):
                @pl.when(_mod(h, up) == part)
                def _():
                    attend((part + 1) * JOB)

            @pl.when(h >= 1)
            def _():
                own, par = out(h - 1)
                own.wait()
                par.wait_send()
                catch_up(h - 1, at_)

            at_ = pump(PLAN_FIRST, 3 * h + 1, at_, h - 1)

            for t in range(n2):
                cols = slice(t * TD, (t + 1) * TD)
                val = _dot(seen[...], wbuf[2, t * qw : (t + 1) * qw])
                v0, v1 = val[:half], val[half:]
                own_st[:, cols] = jnp.where(core == 0, v0, v1)
                par_st[:, cols] = jnp.where(core == 0, v1, v0).astype(BF16)
            for c in out(h):
                c.start()
            return pump(PLAN_FIRST, 3 * h + 2, at_, h - 1)

        lax.fori_loop(0, nh, body, (jnp.int32(0), jnp.int32(0)))
        own, par = out(nh - 1)
        own.wait()
        par.wait_send()
        catch_up(nh - 1, PLAN_CHUNKS[0][0])

    pl.run_scoped(first, pltpu.VMEM((2, JOB, d), BF16), pltpu.VMEM((2, JOB, d), BF16), pltpu.VMEM((JOB, qw), BF16), pltpu.VMEM((length, HEAD), BF16),
                  pltpu.VMEM((length, HEAD), BF16), pltpu.VMEM((JOB, qw), BF16), pltpu.VMEM((half, d), F32), pltpu.VMEM((half, d), BF16),
                  pltpu.VMEM((length, HEAD), F32), pltpu.VMEM((length, HEAD), F32))


    def second(bb, hid, ost, pst):
        def b_copy(first_job, jobs, s):
            return local(G.at[_ds(first_job * JOB, jobs * JOB, JOB)], bb.at[s, pl.ds(0, jobs * JOB)], bsem)

        def outs(first_job, t, q):
            col = _ds(t * TD, TD)
            job = nj + first_job + q
            return (local(ost.at[_mod(t, 2), q], town.at[job, :, col], osem.at[_mod(t, 2), q]),
                    remote(pst.at[_mod(t, 2), q], tpar.at[job, :, col], psem.at[_mod(t, 2), q], exch_recv.at[job], partner))

        def settle(first_job, t, q):
            own, par = outs(first_job, t, q)
            own.wait()
            par.wait_send()

        def chunk(k, first_job, jobs, at_, plan, before, load):
            m = jobs * JOB
            s = _mod(k, 2)
            avail = nj + first_job - 1

            def g_tile(t, at_):
                @pl.when(t < n1 - (SLOTS - 1))
                def _():
                    fetch(k, t + SLOTS - 1)

                @pl.when(t >= n1 - (SLOTS - 1))
                def _():
                    d_copy(k, t + SLOTS - 1).start()

                @pl.when(t == 1)
                def _():
                    for q in range(2):
                        @pl.when(q < before)
                        def _():
                            for u in (n2 - 2, n2 - 1):
                                settle(first_job - before, u, q)

                    for q in (2, 1):
                        @pl.when(q <= before)
                        def _():
                            catch_up(nj + first_job - q, at_)

                for c in g_copies(k, t):
                    c.wait()
                r = _dot(bb[s, :m], wbuf[slot_of(k, t)])
                gate, upv = r[:, :TG], r[:, TG:]
                hid[:m, _ds(t * TG, TG)] = (jax.nn.silu(gate) * upv).astype(BF16)
                at_ = pump(plan, t, at_, jnp.where(t >= 1, avail, avail - before))
                load(t)
                return at_

            at_ = lax.fori_loop(0, n1, g_tile, at_)

            def d_tile(t, at_):
                @pl.when(t < n2 - (SLOTS - 1))
                def _():
                    d_copy(k, n1 + t + SLOTS - 1).start()

                @pl.when((t >= n2 - (SLOTS - 1)) & (k < len(CHUNKS) - 1))
                def _():
                    fetch(k + 1, t + SLOTS - 1 - n2)

                d_copy(k, n1 + t).wait()

                @pl.when(t >= 2)
                def _():
                    for q in range(jobs):
                        settle(first_job, t - 2, q)

                val = _dot(hid[:m], wbuf[slot_of(k, n1 + t), :ff])
                for q in range(jobs):
                    v0, v1 = val[q * JOB : q * JOB + half], val[q * JOB + half : (q + 1) * JOB]
                    ost[_mod(t, 2), q] = jnp.where(core == 0, v0, v1)
                    pst[_mod(t, 2), q] = jnp.where(core == 0, v1, v0).astype(BF16)
                    for c in outs(first_job, t, q):
                        c.start()
                at_ = pump(plan, n1 + t, at_, avail)
                load(n1 + t)
                return at_

            lax.fori_loop(0, n2, d_tile, at_)

        def have(first_job, jobs, s):
            for q in range(jobs):
                gathered(first_job + q)
            b_copy(first_job, jobs, s).start()

        ks = range(len(CHUNKS))

        def body(k, _):
            def pick(f):
                value = jnp.int32(f(0))
                for i in ks[1:]:
                    value = jnp.where(k == i, jnp.int32(f(i)), value)
                return value

            first_job = pick(lambda i: sum(CHUNKS[:i]))
            at_ = tuple(pick(lambda i: PLAN_CHUNKS[i][0][q]) for q in (0, 1))
            plan = [[pick(lambda i: PLAN_CHUNKS[i][2][q][u]) for u in (0, 1)] for q in (0, 1)]
            before = pick(lambda i: CHUNKS[i - 1] if i else 0)
            after = pick(lambda i: CHUNKS[i + 1] if i + 1 < len(CHUNKS) else 0)
            when = pick(lambda i: PLAN_CHUNKS[i][3])
            unread = pick(lambda i: int(i == 0 or PLAN_CHUNKS[i - 1][3] >= ticks))

            for jobs in (1, 2):
                @pl.when(pick(lambda i: CHUNKS[i]) == jobs)
                def _():
                    @pl.when(unread == 1)
                    def _():
                        have(first_job, jobs, _mod(k, 2))

                    b_copy(0, jobs, 0).wait()

                    def load(t):
                        @pl.when(t == when)
                        def _():
                            for q in (1, 2):
                                @pl.when(after == q)
                                def _():
                                    have(first_job + jobs, q, _mod(k + 1, 2))

                    chunk(k, first_job, jobs, at_, plan, before, load)

        lax.fori_loop(0, len(CHUNKS), body, None)
        for q in range(CHUNKS[-1]):
            for u in (n2 - 2, n2 - 1):
                settle(nj - CHUNKS[-1], u, q)

    pl.run_scoped(second, pltpu.VMEM((2, 2 * JOB, d), BF16), pltpu.VMEM((2 * JOB, ff), BF16),
                  pltpu.VMEM((2, 2, half, TD), F32), pltpu.VMEM((2, 2, half, TD), BF16))

    done = PLAN_TAIL[0]
    last = 2 * nj - 1
    catch_up(last, done)
    rs_last_do, ag_last_do = rings(PIECES, True)
    both_from = (chips - 1) * PIECES

    def tail(t, _):
        u = t - both_from
        mixed = (u >= 0) & (u < 2 * PIECES)
        gather = (mixed & (_mod(u, 2) == 1)) | (u >= 2 * PIECES)
        at_ = jnp.where(mixed, _over(u, 2), u - PIECES)

        @pl.when(jnp.logical_not(gather))
        def _():
            i = jnp.where(mixed, both_from + at_, t)
            rs_last_do(jnp.int32(last), _over(i, PIECES), _mod(i, PIECES))

        @pl.when(gather)
        def _():
            ag_last_do(jnp.int32(last), _over(at_, PIECES), _mod(at_, PIECES))

    lax.fori_loop(0, PIECES, tail, None)
    lax.fori_loop(done[1], ended, lambda e, _: ag_event(e), None)
    lax.fori_loop(PIECES, 2 * chips * PIECES, tail, None)
    for j in (2 * nj - 2, 2 * nj - 1):
        for r in range(chips - 1):
            ring_sent(j, r)
        for g in range(chips):
            ag_sent(jnp.int32(j), jnp.int32(g))

    def all_here(j, _):
        gathered(j)

    lax.fori_loop(nj, 2 * nj, all_here, None)


def _copy(start, size, src, dst, buf, get, put):
    n = buf.shape[0]
    ins = [pltpu.make_async_copy(src.at[pl.ds(start + i * size, size)], buf.at[i], get.at[i]) for i in range(n)]
    outs = [pltpu.make_async_copy(buf.at[i], dst.at[pl.ds(i * size, size)], put.at[i]) for i in range(n)]
    for c in ins:
        c.start()
    for i in range(n):
        ins[i].wait()
        outs[i].start()
    for c in outs:
        c.wait()


def solution(mesh):
    n = mesh.shape["tp"]
    chips = n // 2

    def step(x, gain_a, wq, wk, wv, wo, gain_m, w_gate, w_up, w_down):
        batch, length, d = x.shape
        rows, heads, ff = batch * length, wq.shape[1] // HEAD, w_gate.shape[1]
        nj, half, blk = rows // JOB, JOB // 2, JOB // n
        dma, anywhere, vmem = pltpu.SemaphoreType.DMA, pl.BlockSpec(memory_space=pl.ANY), pl.BlockSpec(memory_space=pltpu.VMEM)
        got, _, _ = pl.pallas_call(
            functools.partial(_kernel, n, rows, length, d, heads, ff),
            in_specs=[anywhere, vmem, anywhere, anywhere, anywhere, anywhere, vmem, anywhere, anywhere, anywhere],
            out_specs=[anywhere] * 3,
            out_shape=[jax.ShapeDtypeStruct((2 * rows, d), BF16), jax.ShapeDtypeStruct((2 * nj, half, d), F32),
                       jax.ShapeDtypeStruct((2 * nj, half, d), BF16)],
            scratch_shapes=[
                pltpu.VMEM((2, half, d), F32),
                pltpu.VMEM((2, half, d), BF16),
                pltpu.VMEM((2, blk, d), BF16),
                pltpu.VMEM((4, chips - 1, blk, d), BF16),
                pltpu.VMEM((2, chips - 1, blk, d), BF16),
                pltpu.VMEM((blk, d), F32),
                pltpu.VMEM((4, blk, d), BF16),
                pltpu.VMEM((nj, blk, d), BF16),
                pltpu.VMEM((SLOTS, d, 2 * TG), BF16),
                dma((2 * nj,)),
                dma((2 * nj,)),
                dma((4, chips - 1, HALVES)),
                dma((2, chips - 1)),
                dma((8, chips - 1, HALVES)),
                dma((chips - 1, PIECES)),
                dma((chips - 1, PIECES)),
                dma((2, chips)),
                dma((2, chips)),
                dma((2,)),
                dma((2, 3)),
                dma((SLOTS, 2)),
                dma(()),
                dma((2, 2)),
                dma((2, 2)),
                dma((3 + d // TD,)),
                dma((2,)),
                pltpu.VMEM((2, d), F32),
            ],
            compiler_params=pltpu.CompilerParams(collective_id=0, has_side_effects=True, vmem_limit_bytes=67043328),
            name="layer",
        )(x.reshape(rows, d), gain_a, wq, wk, wv, wo, gain_m, w_gate, w_up, w_down)
        y = pl.pallas_call(
            functools.partial(_copy, rows, rows // 4),
            in_specs=[anywhere],
            out_specs=anywhere,
            out_shape=jax.ShapeDtypeStruct((rows, d), BF16),
            scratch_shapes=[pltpu.VMEM((4, rows // 4, d), BF16), dma((4,)), dma((4,))],
            name="copy_out",
        )(got)
        return y.reshape(x.shape)

    tokens, whole, columns, rows_of = P("dp", None, None), P(None), P(None, "tp"), P("tp", None)
    return jax.shard_map(
        step,
        mesh=mesh,
        in_specs=(tokens, whole, columns, columns, columns, rows_of, whole, columns, columns, rows_of),
        out_specs=tokens,
        check_vma=False,
    )
```

```python
import functools

import jax
import jax.numpy as jnp
from jax import lax
from jax.experimental import pallas as pl
from jax.experimental.pallas import tpu as pltpu
from jax.sharding import PartitionSpec as P

HEAD = 128
THETA = 10000
JOB = 256
TG = 256
TD = 512
SLOTS = 4
HALVES = 2
PIECES = 4
CHUNKS = (1, 1, 2, 2, 1, 1)
PLAN_FIRST = ((34949120, 1131010), (33554432, 332880))
PLAN_CHUNKS = (
    ((15, 8), (0, 0), ((69653, 17317905), (5243202, 17056832)), 20),
    ((26, 19), (0, 0), ((263172, 2098177), (16793664, 1179712)), 23),
    ((33, 26), (0, 0), ((25445397, 4260929), (23138565, 1065232)), 11),
    ((47, 39), (0, 0), ((1118296, 17), (17056790, 18105624)), 0),
    ((56, 56), (0, 0), ((17055872, 4164), (0, 17043520)), 0),
    ((64, 60), (0, 0), ((8409216, 20), (1052740, 17895456)), 99),
)
PLAN_TAIL = ((72, 70), 18, 261129)
HIDDEN = -1e30
F32, BF16 = jnp.float32, jnp.bfloat16


def _dot(a, b, ca=1, cb=0):
    return lax.dot_general(a, b, (((ca,), (cb,)), ((), ())), preferred_element_type=F32)


def _mod(a, n):
    return a & (n - 1)


def _over(a, n):
    return a >> (n.bit_length() - 1)


def _ds(start, size, unit=128):
    return pl.ds(pl.multiple_of(start, unit), size)


def _kernel(n, rows, length, d, heads, ff, *refs):
    (x, ga, wq, wk, wv, wo, gm, wg, wu, wd, G, town, tpar,
     tv_own, tv_par, xres, rrecv, rsend, fin, gout, hown, wbuf,
     exch_recv, agp_recv, rs_recv, rs_send, ag_recv, rs_last, ag_last, ag_sn, ag_sp, agl, tl, gsem, bsem, osem, psem, wsem, xsem, gains) = refs
    chips, half, blk = n // 2, JOB // 2, JOB // n
    nj = rows // JOB
    per = HALVES * chips
    half_plan = 13
    qw = heads * HEAD
    me = lax.axis_index("tp")
    chip, core = _over(me, 2), _mod(me, 2)
    step = 1 - 2 * core
    at = lambda c, k: _mod(c + chips, chips) * 2 + k
    nxt, prv, partner = at(chip + step, core), at(chip - step, core), at(chip, 1 - core)

    barrier = pltpu.get_barrier_semaphore()
    for other in (nxt, prv, partner):
        pl.semaphore_signal(barrier, inc=1, device_id={"tp": other}, device_id_type=pl.DeviceIdType.MESH)

    gains[0:1] = ga[...].astype(F32).reshape(1, d)
    gains[1:2] = gm[...].astype(F32).reshape(1, d)

    def remote(src, dst, send, recv, to):
        return pltpu.make_async_remote_copy(src_ref=src, dst_ref=dst, send_sem=send, recv_sem=recv, device_id={"tp": to},
                                            device_id_type=pl.DeviceIdType.MESH)

    local = pltpu.make_async_copy

    early = 2 * per
    late = early + (nj - 2) * per
    ended = late + per

    def alone(e):
        return (e < early) | (e >= late)

    def event(e):
        single = jnp.where(e < early, _over(e, per), 2 * nj - 2)
        return jnp.where(alone(e), single, 2 + 2 * _over(e - early, per) + _mod(e, 2)), _mod(_over(e, 2), chips), _mod(e, 2)

    def last_event(j):
        paired = early + per * (_over(j, 2) - 1) + per - 2 + _mod(j, 2)
        return jnp.where(j < 2, per * j + per - 1, jnp.where(j < 2 * nj - 2, paired, late + per - 1))

    def loads(j):
        p = _mod(j, 2)
        mine = _ds(_mod(j, nj) * JOB + core * half + chip * blk, blk, blk)
        return (local(town.at[j], tv_own.at[p], tl.at[p, 0]), local(tpar.at[j], tv_par.at[p], tl.at[p, 1]),
                local(x.at[mine], xres.at[p], tl.at[p, 2]))

    def exchanged(j):
        return remote(tpar.at[j], tpar.at[j], psem.at[0, 0], exch_recv.at[j], partner)

    def tload(j):
        exchanged(j).wait_recv()
        for c in loads(j):
            c.start()

    def ring_sent(j, r):
        remote(rsend.at[_mod(j, 2), r], rrecv.at[_mod(j, 4), r], rs_send.at[_mod(j, 2), r], rs_recv.at[_mod(j, 4), r, 0], nxt).wait_send()

    def block(j, g):
        o = _mod(chip - step * g + chips * 2, chips)
        return _ds(j * JOB + core * half + o * blk, blk, blk)

    def to_partner(j, g, src):
        return remote(src, G.at[block(j, g)], ag_sp.at[_mod(j, 2), g], agp_recv.at[j], partner)

    def keep(j):
        return local(gout.at[_mod(j, 4)], G.at[block(j, 0)], agl.at[_mod(j, 2)])

    def ag_sent(j, g):
        whole = G.at[block(j, g)]
        to_partner(j, g, whole).wait_send()

        @pl.when(g < chips - 1)
        def _():
            remote(whole, whole, ag_sn.at[_mod(j, 2), g], ag_recv.at[_mod(j, 8), g, 0], nxt).wait_send()

    def finish(j):
        idx, p = _mod(j, nj), _mod(j, 2)

        @pl.when(j < nj)
        def _():
            h = (xres[p].astype(F32) + fin[...]).astype(BF16)
            hown[idx] = h
            wide = h.astype(F32)
            scale = lax.rsqrt(jnp.mean(wide * wide, -1, keepdims=True) + 1e-6)
            gout[_mod(j, 4)] = (wide * scale * gains[1:2]).astype(BF16)

        @pl.when(j >= nj)
        def _():
            gout[_mod(j, 4)] = (hown[idx].astype(F32) + fin[...]).astype(BF16)

    def rings(pieces, last):
        cw = d // pieces
        cols_of = lambda c: pl.ds(0, d) if pieces == 1 else _ds(c * cw, cw)
        rs_at = (lambda j, r, c: rs_last.at[r, c]) if last else (lambda j, r, c: rs_recv.at[_mod(j, 4), r, c])
        ag_at = (lambda j, g, c: ag_last.at[g, c]) if last else (lambda j, g, c: ag_recv.at[_mod(j, 8), g, c])

        def ring(j, r, c):
            return remote(rsend.at[_mod(j, 2), r, :, cols_of(c)], rrecv.at[_mod(j, 4), r, :, cols_of(c)], rs_send.at[_mod(j, 2), r],
                          rs_at(j, r, c), nxt)

        def rs_do(j, r, c, avail=None):
            p = _mod(j, 2)
            o = _mod(chip + step * (chips - 1 - r) + chips * 2, chips)
            there = _ds(o * blk, blk, blk)

            @pl.when((r == 0) & (c == 0))
            def _():
                for copy in loads(j):
                    copy.wait()

            def both(cols):
                return tv_own[p, there, cols] + tv_par[p, there, cols].astype(F32)

            def all_(cols):
                return both(cols) + rrecv[_mod(j, 4), r - 1, :, cols].astype(F32)

            def send(total):
                @pl.when((j >= 2) & (c == 0))
                def _():
                    ring_sent(j - 2, r)

                rsend[p, r, :, cols_of(c)] = total(cols_of(c)).astype(BF16)
                ring(j, r, c).start()

            @pl.when(r == 0)
            def _():
                send(both)

            @pl.when(r > 0)
            def _():
                ring(j, r - 1, c).wait_recv()

            @pl.when((r > 0) & (r < chips - 1))
            def _():
                send(all_)

            @pl.when(r == chips - 1)
            def _():
                cols = cols_of(c)
                if last:
                    gout[_mod(j, 4), :, cols] = (hown[_mod(j, nj), :, cols].astype(F32) + all_(cols)).astype(BF16)
                else:
                    fin[:, cols] = all_(cols)

            if not last:
                @pl.when((r == chips - 1) & (c == pieces - 1))
                def _():
                    finish(j)

                    @pl.when(j + 2 <= avail)
                    def _():
                        tload(j + 2)

        def to_next(j, g, c, src):
            return remote(src, G.at[block(j, g), cols_of(c)], ag_sn.at[_mod(j, 2), g], ag_at(j, g, c), nxt)

        def ag_do(j, g, c):
            here = G.at[block(j, g), cols_of(c)]

            @pl.when((j >= 2) & (c == 0))
            def _():
                ag_sent(j - 2, g)

            @pl.when(g == 0)
            def _():
                to_next(j, g, c, gout.at[_mod(j, 4), :, cols_of(c)]).start()

                @pl.when(c == pieces - 1)
                def _():
                    to_partner(j, g, gout.at[_mod(j, 4)]).start()
                    keep(j).start()

            @pl.when(g > 0)
            def _():
                to_next(j, g - 1, c, here).wait_recv()

                @pl.when(g < chips - 1)
                def _():
                    to_next(j, g, c, here).start()

                @pl.when(c == pieces - 1)
                def _():
                    to_partner(j, g, G.at[block(j, g)]).start()

                    @pl.when(g == chips - 1)
                    def _():
                        keep(j).wait()

        return rs_do, ag_do

    rs_piece, ag_piece = rings(HALVES, False)
    rs_whole, ag_whole = rings(1, False)

    def rs_event(e, avail):
        j, r, which = event(e)

        @pl.when(alone(e))
        def _():
            rs_piece(j, r, which, avail)

        @pl.when(jnp.logical_not(alone(e)))
        def _():
            rs_whole(j, r, 0, avail)

    def ag_event(e):
        j, g, which = event(e)

        @pl.when(alone(e))
        def _():
            ag_piece(j, g, which)

        @pl.when(jnp.logical_not(alone(e)))
        def _():
            ag_whole(j, g, 0)

    def gathered(j):
        there = G.at[_ds(j * JOB, half, half)]
        remote(there, there, ag_sp.at[0, 0], agp_recv.at[j], partner).wait_recv()

    def pump(plan, t, at_, avail):
        (a0, a1), (b0, b1) = plan
        u = 2 * jnp.where(t < half_plan, t, t - half_plan)
        a = lax.shift_right_logical(jnp.where(t < half_plan, a0, a1), u) & 3
        b = lax.shift_right_logical(jnp.where(t < half_plan, b0, b1), u) & 3
        r, g = at_
        lax.fori_loop(r, r + a, lambda e, _: rs_event(e, avail), None)
        lax.fori_loop(g, g + b, lambda e, _: ag_event(e), None)
        return r + a, g + b

    def catch_up(j, at_):
        @pl.when((j < 2) | (last_event(j - 2) < at_[0]))
        def _():
            tload(j)

    n1, n2 = ff // TG, d // TD
    ticks = n1 + n2
    slot_of = lambda k, t: _mod(k * ticks + 3 + t, SLOTS)

    def g_copies(k, t):
        col, s = _ds(t * TG, TG), slot_of(k, t)
        return (local(wg.at[:, col], wbuf.at[s, :, pl.ds(0, TG)], gsem.at[s, 0]),
                local(wu.at[:, col], wbuf.at[s, :, pl.ds(TG, TG)], gsem.at[s, 1]))

    def d_copy(k, t):
        s = slot_of(k, t)
        return local(wd.at[:, _ds((t - n1) * TD, TD)], wbuf.at[s, pl.ds(0, ff)], gsem.at[s, 0])

    def fetch(k, t):
        for c in g_copies(k, t):
            c.start()

    def first(xb, ab, qb, kb, vb, seen, own_st, par_st, cos, sin):
        nh = rows // JOB
        up = length // JOB
        wcopies = [local(wq, wbuf.at[0], wsem.at[0]), local(wk, wbuf.at[1, :, pl.ds(0, HEAD)], wsem.at[1]),
                   local(wv, wbuf.at[1, :, pl.ds(HEAD, HEAD)], wsem.at[2])]
        wcopies += [local(wo.at[:, pl.ds(t * TD, TD)], wbuf.at[2, pl.ds(t * qw, qw)], wsem.at[3 + t]) for t in range(n2)]
        x_copy = lambda h: local(x.at[_ds(h * JOB, JOB, JOB)], xb.at[_mod(h, 2)], xsem.at[_mod(h, 2)])
        x_copy(0).start()
        for c in wcopies[:3]:
            c.start()
        lane = lax.broadcasted_iota(jnp.int32, (16, HEAD), 1)
        row = lax.broadcasted_iota(jnp.int32, (16, HEAD), 0).astype(F32)
        power = jnp.exp((lane % (HEAD // 2)).astype(F32) * (-2.0 / HEAD) * jnp.log(jnp.float32(THETA)))
        sign = jnp.where(lane < HEAD // 2, -1.0, 1.0)
        cf, sf = jnp.cos(row * power), jnp.sin(row * power)
        for a in range(0, length, 256):
            cc, sc = jnp.cos((16 * row + a) * power), jnp.sin((16 * row + a) * power)
            for i in range(16):
                at_ = slice(a + 16 * i, a + 16 * (i + 1))
                ci, si = cc[i : i + 1], sc[i : i + 1]
                cos[at_, :] = ci * cf - si * sf
                sin[at_, :] = sign * (si * cf + ci * sf)

        def out(h):
            return (local(own_st, town.at[h], osem.at[0, 0]), remote(par_st, tpar.at[h], psem.at[0, 0], exch_recv.at[h], partner))

        def normed(h):
            for a in range(0, JOB, 16):
                rows_ = slice(a, a + 16)
                wide = xb[_mod(h, 2), rows_, :].astype(F32)
                scale = lax.rsqrt(jnp.mean(wide * wide, -1, keepdims=True) + 1e-6)
                ab[_mod(h, 2), rows_, :] = (xb[_mod(h, 2), rows_, :].astype(F32) * scale * gains[0:1]).astype(BF16)

        x_copy(0).wait()
        normed(0)
        x_copy(1).start()
        for c in wcopies[:3]:
            c.wait()
        for c in wcopies[3:]:
            c.start()

        pl.semaphore_wait(barrier, 3)

        def body(h, at_):
            at_seq = (_mod(h, up)) * JOB

            @pl.when(h + 1 < nh)
            def _():
                x_copy(h + 1).wait()

            here = _ds(at_seq, JOB, JOB)
            cosv, sinv = cos[here, :], sin[here, :]

            def turned(t):
                t = t.astype(BF16).astype(F32)
                return (t * cosv + pltpu.roll(t, HEAD // 2, 1) * sinv).astype(BF16)

            queries = _dot(ab[_mod(h, 2)], wbuf[0])
            others = _dot(ab[_mod(h, 2)], wbuf[1, :, : 2 * HEAD])
            normed(h + 1)
            kb[here, :] = turned(others[:, :HEAD])
            vb[here, :] = others[:, HEAD:].astype(BF16)
            for m in range(heads):
                qb[:, m * HEAD : (m + 1) * HEAD] = turned(queries[:, m * HEAD : (m + 1) * HEAD])

            @pl.when(h + 2 < nh)
            def _():
                x_copy(h + 2).start()

            @pl.when(h == nh - 1)
            def _():
                fetch(0, 1)
                fetch(0, 2)

            @pl.when(h == 0)
            def _():
                for c in wcopies[3:]:
                    c.wait()

            @pl.when(h == 3)
            def _():
                fetch(0, 0)

            at_ = pump(PLAN_FIRST, 3 * h, at_, h - 2)

            def attend(keys):
                ok = (keys - JOB + lax.broadcasted_iota(jnp.int32, (JOB, keys), 0)) >= lax.broadcasted_iota(jnp.int32, (JOB, keys), 1)
                for m in range(heads):
                    s = _dot(qb[:, m * HEAD : (m + 1) * HEAD], kb[:keys], 1, 1)
                    s = jnp.where(ok, s, HIDDEN)
                    w = jnp.exp2((s - s.max(-1, keepdims=True)) * (HEAD**-0.5 * 1.4426950408889634))
                    total = w.sum(-1, keepdims=True)
                    seen[:, m * HEAD : (m + 1) * HEAD] = (_dot(w.astype(BF16), vb[:keys]) / total).astype(BF16)

            for part in range(up):
                @pl.when(_mod(h, up) == part)
                def _():
                    attend((part + 1) * JOB)

            @pl.when(h >= 1)
            def _():
                own, par = out(h - 1)
                own.wait()
                par.wait_send()
                catch_up(h - 1, at_)

            at_ = pump(PLAN_FIRST, 3 * h + 1, at_, h - 1)

            for t in range(n2):
                cols = slice(t * TD, (t + 1) * TD)
                val = _dot(seen[...], wbuf[2, t * qw : (t + 1) * qw])
                v0, v1 = val[:half], val[half:]
                own_st[:, cols] = jnp.where(core == 0, v0, v1)
                par_st[:, cols] = jnp.where(core == 0, v1, v0).astype(BF16)
            for c in out(h):
                c.start()
            return pump(PLAN_FIRST, 3 * h + 2, at_, h - 1)

        lax.fori_loop(0, nh, body, (jnp.int32(0), jnp.int32(0)))
        own, par = out(nh - 1)
        own.wait()
        par.wait_send()
        catch_up(nh - 1, PLAN_CHUNKS[0][0])

    pl.run_scoped(first, pltpu.VMEM((2, JOB, d), BF16), pltpu.VMEM((2, JOB, d), BF16), pltpu.VMEM((JOB, qw), BF16), pltpu.VMEM((length, HEAD), BF16),
                  pltpu.VMEM((length, HEAD), BF16), pltpu.VMEM((JOB, qw), BF16), pltpu.VMEM((half, d), F32), pltpu.VMEM((half, d), BF16),
                  pltpu.VMEM((length, HEAD), F32), pltpu.VMEM((length, HEAD), F32))


    def second(bb, hid, ost, pst):
        def b_copy(first_job, jobs, s):
            return local(G.at[_ds(first_job * JOB, jobs * JOB, JOB)], bb.at[s, pl.ds(0, jobs * JOB)], bsem)

        def outs(first_job, t, q):
            col = _ds(t * TD, TD)
            job = nj + first_job + q
            return (local(ost.at[_mod(t, 2), q], town.at[job, :, col], osem.at[_mod(t, 2), q]),
                    remote(pst.at[_mod(t, 2), q], tpar.at[job, :, col], psem.at[_mod(t, 2), q], exch_recv.at[job], partner))

        def settle(first_job, t, q):
            own, par = outs(first_job, t, q)
            own.wait()
            par.wait_send()

        def chunk(k, first_job, jobs, at_, plan, before, load):
            m = jobs * JOB
            s = _mod(k, 2)
            avail = nj + first_job - 1

            def g_tile(t, at_):
                @pl.when(t < n1 - (SLOTS - 1))
                def _():
                    fetch(k, t + SLOTS - 1)

                @pl.when(t >= n1 - (SLOTS - 1))
                def _():
                    d_copy(k, t + SLOTS - 1).start()

                @pl.when(t == 1)
                def _():
                    for q in range(2):
                        @pl.when(q < before)
                        def _():
                            for u in (n2 - 2, n2 - 1):
                                settle(first_job - before, u, q)

                    for q in (2, 1):
                        @pl.when(q <= before)
                        def _():
                            catch_up(nj + first_job - q, at_)

                for c in g_copies(k, t):
                    c.wait()
                r = _dot(bb[s, :m], wbuf[slot_of(k, t)])
                gate, upv = r[:, :TG], r[:, TG:]
                hid[:m, _ds(t * TG, TG)] = (jax.nn.silu(gate) * upv).astype(BF16)
                at_ = pump(plan, t, at_, jnp.where(t >= 1, avail, avail - before))
                load(t)
                return at_

            at_ = lax.fori_loop(0, n1, g_tile, at_)

            def d_tile(t, at_):
                @pl.when(t < n2 - (SLOTS - 1))
                def _():
                    d_copy(k, n1 + t + SLOTS - 1).start()

                @pl.when((t >= n2 - (SLOTS - 1)) & (k < len(CHUNKS) - 1))
                def _():
                    fetch(k + 1, t + SLOTS - 1 - n2)

                d_copy(k, n1 + t).wait()

                @pl.when(t >= 2)
                def _():
                    for q in range(jobs):
                        settle(first_job, t - 2, q)

                val = _dot(hid[:m], wbuf[slot_of(k, n1 + t), :ff])
                for q in range(jobs):
                    v0, v1 = val[q * JOB : q * JOB + half], val[q * JOB + half : (q + 1) * JOB]
                    ost[_mod(t, 2), q] = jnp.where(core == 0, v0, v1)
                    pst[_mod(t, 2), q] = jnp.where(core == 0, v1, v0).astype(BF16)
                    for c in outs(first_job, t, q):
                        c.start()
                at_ = pump(plan, n1 + t, at_, avail)
                load(n1 + t)
                return at_

            lax.fori_loop(0, n2, d_tile, at_)

        def have(first_job, jobs, s):
            for q in range(jobs):
                gathered(first_job + q)
            b_copy(first_job, jobs, s).start()

        ks = range(len(CHUNKS))

        def body(k, _):
            def pick(f):
                value = jnp.int32(f(0))
                for i in ks[1:]:
                    value = jnp.where(k == i, jnp.int32(f(i)), value)
                return value

            first_job = pick(lambda i: sum(CHUNKS[:i]))
            at_ = tuple(pick(lambda i: PLAN_CHUNKS[i][0][q]) for q in (0, 1))
            plan = [[pick(lambda i: PLAN_CHUNKS[i][2][q][u]) for u in (0, 1)] for q in (0, 1)]
            before = pick(lambda i: CHUNKS[i - 1] if i else 0)
            after = pick(lambda i: CHUNKS[i + 1] if i + 1 < len(CHUNKS) else 0)
            when = pick(lambda i: PLAN_CHUNKS[i][3])
            unread = pick(lambda i: int(i == 0 or PLAN_CHUNKS[i - 1][3] >= ticks))

            for jobs in (1, 2):
                @pl.when(pick(lambda i: CHUNKS[i]) == jobs)
                def _():
                    @pl.when(unread == 1)
                    def _():
                        have(first_job, jobs, _mod(k, 2))

                    b_copy(0, jobs, 0).wait()

                    def load(t):
                        @pl.when(t == when)
                        def _():
                            for q in (1, 2):
                                @pl.when(after == q)
                                def _():
                                    have(first_job + jobs, q, _mod(k + 1, 2))

                    chunk(k, first_job, jobs, at_, plan, before, load)

        lax.fori_loop(0, len(CHUNKS), body, None)
        for q in range(CHUNKS[-1]):
            for u in (n2 - 2, n2 - 1):
                settle(nj - CHUNKS[-1], u, q)

    pl.run_scoped(second, pltpu.VMEM((2, 2 * JOB, d), BF16), pltpu.VMEM((2 * JOB, ff), BF16),
                  pltpu.VMEM((2, 2, half, TD), F32), pltpu.VMEM((2, 2, half, TD), BF16))

    done = PLAN_TAIL[0]
    last = 2 * nj - 1
    catch_up(last, done)
    rs_last_do, ag_last_do = rings(PIECES, True)
    both_from = (chips - 1) * PIECES

    def tail(t, _):
        u = t - both_from
        mixed = (u >= 0) & (u < 2 * PIECES)
        gather = (mixed & (_mod(u, 2) == 1)) | (u >= 2 * PIECES)
        at_ = jnp.where(mixed, _over(u, 2), u - PIECES)

        @pl.when(jnp.logical_not(gather))
        def _():
            i = jnp.where(mixed, both_from + at_, t)
            rs_last_do(jnp.int32(last), _over(i, PIECES), _mod(i, PIECES))

        @pl.when(gather)
        def _():
            ag_last_do(jnp.int32(last), _over(at_, PIECES), _mod(at_, PIECES))

    lax.fori_loop(0, PIECES, tail, None)
    lax.fori_loop(done[1], ended, lambda e, _: ag_event(e), None)
    lax.fori_loop(PIECES, 2 * chips * PIECES, tail, None)
    for j in (2 * nj - 2, 2 * nj - 1):
        for r in range(chips - 1):
            ring_sent(j, r)
        for g in range(chips):
            ag_sent(jnp.int32(j), jnp.int32(g))

    def all_here(j, _):
        gathered(j)

    lax.fori_loop(nj, 2 * nj, all_here, None)


def _copy(start, size, src, dst, buf, get, put):
    n = buf.shape[0]
    ins = [pltpu.make_async_copy(src.at[pl.ds(start + i * size, size)], buf.at[i], get.at[i]) for i in range(n)]
    outs = [pltpu.make_async_copy(buf.at[i], dst.at[pl.ds(i * size, size)], put.at[i]) for i in range(n)]
    for c in ins:
        c.start()
    for i in range(n):
        ins[i].wait()
        outs[i].start()
    for c in outs:
        c.wait()


def solution(mesh):
    n = mesh.shape["tp"]
    chips = n // 2

    def step(x, gain_a, wq, wk, wv, wo, gain_m, w_gate, w_up, w_down):
        batch, length, d = x.shape
        rows, heads, ff = batch * length, wq.shape[1] // HEAD, w_gate.shape[1]
        nj, half, blk = rows // JOB, JOB // 2, JOB // n
        dma, anywhere, vmem = pltpu.SemaphoreType.DMA, pl.BlockSpec(memory_space=pl.ANY), pl.BlockSpec(memory_space=pltpu.VMEM)
        got, _, _ = pl.pallas_call(
            functools.partial(_kernel, n, rows, length, d, heads, ff),
            in_specs=[anywhere, vmem, anywhere, anywhere, anywhere, anywhere, vmem, anywhere, anywhere, anywhere],
            out_specs=[anywhere] * 3,
            out_shape=[jax.ShapeDtypeStruct((2 * rows, d), BF16), jax.ShapeDtypeStruct((2 * nj, half, d), F32),
                       jax.ShapeDtypeStruct((2 * nj, half, d), BF16)],
            scratch_shapes=[
                pltpu.VMEM((2, half, d), F32),
                pltpu.VMEM((2, half, d), BF16),
                pltpu.VMEM((2, blk, d), BF16),
                pltpu.VMEM((4, chips - 1, blk, d), BF16),
                pltpu.VMEM((2, chips - 1, blk, d), BF16),
                pltpu.VMEM((blk, d), F32),
                pltpu.VMEM((4, blk, d), BF16),
                pltpu.VMEM((nj, blk, d), BF16),
                pltpu.VMEM((SLOTS, d, 2 * TG), BF16),
                dma((2 * nj,)),
                dma((2 * nj,)),
                dma((4, chips - 1, HALVES)),
                dma((2, chips - 1)),
                dma((8, chips - 1, HALVES)),
                dma((chips - 1, PIECES)),
                dma((chips - 1, PIECES)),
                dma((2, chips)),
                dma((2, chips)),
                dma((2,)),
                dma((2, 3)),
                dma((SLOTS, 2)),
                dma(()),
                dma((2, 2)),
                dma((2, 2)),
                dma((3 + d // TD,)),
                dma((2,)),
                pltpu.VMEM((2, d), F32),
            ],
            compiler_params=pltpu.CompilerParams(collective_id=0, has_side_effects=True, vmem_limit_bytes=67043328),
            name="layer",
        )(x.reshape(rows, d), gain_a, wq, wk, wv, wo, gain_m, w_gate, w_up, w_down)
        y = pl.pallas_call(
            functools.partial(_copy, rows, rows // 4),
            in_specs=[anywhere],
            out_specs=anywhere,
            out_shape=jax.ShapeDtypeStruct((rows, d), BF16),
            scratch_shapes=[pltpu.VMEM((4, rows // 4, d), BF16), dma((4,)), dma((4,))],
            name="copy_out",
        )(got)
        return y.reshape(x.shape)

    tokens, whole, columns, rows_of = P("dp", None, None), P(None), P(None, "tp"), P("tp", None)
    return jax.shard_map(
        step,
        mesh=mesh,
        in_specs=(tokens, whole, columns, columns, columns, rows_of, whole, columns, columns, rows_of),
        out_specs=tokens,
        check_vma=False,
    )
```
